1024 devices in a mesh: tiles: 256 (over x, z, core), strip: 4 (over y).
Axes of the slice: x: 4, y: 4, z: 32, core: 2. Of those that a mesh axis runs over, the one named last changes fastest.
Arguments:
- fields: float32 [256, 4, 3, 3, 4, 8100], P('tiles', 'strip'), may hold values from -6 to 6
- wet_land: int32 [256, 4, 3, 8100], P('tiles', 'strip'), may hold values from 0 to 1, as said below
- links: int32 [256, 4, 3, 4, 4], P('tiles', 'strip'), may hold values from -1 to 3, as said below
- surface_diagonal: float32 [256, 4, 3, 8100], P('tiles', 'strip'), may hold values from 0.25 to 2
- spread: float32 [3, 4], replicated, may hold values from 0.02 to 0.2
- mixing: float32 [4], replicated, may hold values from 0.02 to 0.2
- thickness: float32 [4], replicated, may hold values from 0.5 to 2
Outputs:
- adjoint_fields: float32 [256, 4, 3, 3, 4, 8100], P('tiles', 'strip')
- surface_solution: float32 [256, 4, 3, 8100], P('tiles', 'strip')
- surface_residual: float32 [256, 4, 3, 8100], P('tiles', 'strip')
The draws below stay inside these ranges and needn't reach their ends.
Inputs may be any that keep to these rules, and one draw needn't show every extreme that they name: wet_land is 1 on most cells of the first 1 to 3 slots of each device and 0 on all cells of its other slots. Offsets dt and ds are -1, 0 or 1; on the west and east sides dt is -1 and 1, on the south and north sides ds is -1 and 1; a partner slot is -1 or a slot that holds wet cells; links are mutual: side e of slot k pairs with side e XOR 1 of its partner, whose entry points back with opposite offsets and rotation code (4 - code) mod 4; an empty slot has no links; rotation codes are 0 to 3.
All inputs are finite; a program needn't handle non-finite values.
Results may differ from the reference program's by a relative error of at most 0.00027.
Values sent between devices are 32-bit elements; how exact they have to be, the bound alone decides.
A program may use at most 64 MiB of HBM per device.

```python
import math
import jax
import jax.numpy as jnp
import numpy as np
from jax import lax

TILE = 90
SLOTS = 3
FIELDS = 3
LEVELS = 4
ITERS = 2
CELLS = 8100
TILE_GROUPS = 256
STRIP_GROUPS = 4


def wet_counts(key):
    return jax.random.randint(jax.random.fold_in(key, 11), (TILE_GROUPS, STRIP_GROUPS), 1, SLOTS + 1)


def live_slots(key):
    counts = wet_counts(key)
    return jnp.arange(SLOTS, dtype=jnp.int32)[None, None, :] < counts[:, :, None]


def draw_wet_land(key, part):
    live = live_slots(key)
    ocean = jax.random.randint(jax.random.fold_in(key, 13), (TILE_GROUPS, STRIP_GROUPS, SLOTS, CELLS), 0, 8) != 0
    return (live[..., None] & ocean).astype(jnp.int32)


def slot_orders(key):
    scores = jax.random.randint(key, (TILE_GROUPS, STRIP_GROUPS, SLOTS), 0, 1 << 20) * SLOTS
    scores = scores + jnp.arange(SLOTS, dtype=jnp.int32)[None, None, :]
    order = jnp.argsort(scores, axis=-1).astype(jnp.int32)
    inverse = jnp.argsort(order, axis=-1).astype(jnp.int32)
    return (order, inverse)


def entry_table(group_shift, strip_shift, partner, code):
    shape = (TILE_GROUPS, STRIP_GROUPS, SLOTS)
    return jnp.stack([jnp.broadcast_to(group_shift, shape), jnp.broadcast_to(strip_shift, shape), jnp.broadcast_to(partner, shape), jnp.broadcast_to(code, shape)], axis=-1).astype(jnp.int32)


def draw_links(key, part):
    live = live_slots(key)
    shape = (TILE_GROUPS, STRIP_GROUPS, SLOTS)
    group_ids = jnp.arange(TILE_GROUPS, dtype=jnp.int32)[:, None, None]
    strip_ids = jnp.arange(STRIP_GROUPS, dtype=jnp.int32)[None, :, None]
    slot_ids = jnp.arange(SLOTS, dtype=jnp.int32)[None, None, :]
    east_shift = jax.random.randint(jax.random.fold_in(key, 21), (TILE_GROUPS,), -1, 2)
    east_order, east_inverse = slot_orders(jax.random.fold_in(key, 22))
    east_code = jax.random.randint(jax.random.fold_in(key, 23), shape, 0, 4)
    east_cut = jax.random.randint(jax.random.fold_in(key, 24), shape, 0, 8) == 0
    east_group = (group_ids + 1) % TILE_GROUPS
    east_strip = (strip_ids + east_shift[:, None, None]) % STRIP_GROUPS
    east_live = live & live[east_group, east_strip, east_order] & jnp.logical_not(east_cut)
    east_entry = entry_table(1, east_shift[:, None, None], jnp.where(east_live, east_order, -1), east_code)
    from_group = (group_ids - 1) % TILE_GROUPS
    west_shift = east_shift[from_group]
    from_strip = (strip_ids - west_shift) % STRIP_GROUPS
    from_slot = east_inverse[from_group, from_strip, slot_ids]
    west_live = east_live[from_group, from_strip, from_slot]
    west_code = (4 - east_code[from_group, from_strip, from_slot]) % 4
    west_entry = entry_table(-1, -west_shift, jnp.where(west_live, from_slot, -1), west_code)
    north_shift = jax.random.randint(jax.random.fold_in(key, 31), (STRIP_GROUPS,), -1, 2)
    north_order, north_inverse = slot_orders(jax.random.fold_in(key, 32))
    north_code = jax.random.randint(jax.random.fold_in(key, 33), shape, 0, 4)
    north_cut = jax.random.randint(jax.random.fold_in(key, 34), shape, 0, 8) == 0
    north_group = (group_ids + north_shift[None, :, None]) % TILE_GROUPS
    north_strip = (strip_ids + 1) % STRIP_GROUPS
    north_live = live & live[north_group, north_strip, north_order] & jnp.logical_not(north_cut)
    north_entry = entry_table(north_shift[None, :, None], 1, jnp.where(north_live, north_order, -1), north_code)
    below_strip = (strip_ids - 1) % STRIP_GROUPS
    south_shift = north_shift[below_strip]
    below_group = (group_ids - south_shift) % TILE_GROUPS
    below_slot = north_inverse[below_group, below_strip, slot_ids]
    south_live = north_live[below_group, below_strip, below_slot]
    south_code = (4 - north_code[below_group, below_strip, below_slot]) % 4
    south_entry = entry_table(-south_shift, -1, jnp.where(south_live, below_slot, -1), south_code)
    return jnp.stack([west_entry, east_entry, south_entry, north_entry], axis=3)


def steps_of(stream_key, dims, cuts, low, largest):
    def one(position, blocks):
        draws = jax.random.uniform(jax.random.fold_in(jax.random.fold_in(stream_key, 6), position), (blocks,), jnp.float32, low / len(cuts), largest / len(cuts))
        return jnp.repeat(jnp.exp(draws), dims[position] // blocks).reshape((-1,) + (1,) * (len(dims) - position - 1))

    level = one(*cuts[0])
    for cut in cuts[1:]:
        level = level * one(*cut)
    return level


def scatter_about(key, extent, scale, bound, cuts=(), kind=jnp.bfloat16):
    gain = steps_of(key, extent, cuts, -0.22, 0.18) if cuts else 1.0
    values = jax.random.normal(key, extent, jnp.float32) * scale * gain
    return jnp.minimum(jnp.maximum(values, -bound), bound).astype(kind)


def setup_inputs(seed: int = 0) -> dict:
    key_list = jax.random.split(jax.random.key(seed), 8)
    return {
        "fields": scatter_about(key_list[0], (TILE_GROUPS, STRIP_GROUPS, SLOTS, FIELDS, LEVELS, CELLS), 1.0, 6.0, ((0, 256), (1, 4)), jnp.float32),
        "wet_land": draw_wet_land(jax.random.fold_in(key_list[7], 71), 0),
        "links": draw_links(jax.random.fold_in(key_list[7], 71), 0),
        "surface_diagonal": jnp.clip(0.25 + 1.75 * jax.random.uniform(key_list[3], (TILE_GROUPS, STRIP_GROUPS, SLOTS, CELLS), jnp.float32) ** steps_of(key_list[3], (TILE_GROUPS, STRIP_GROUPS, SLOTS, CELLS), ((0, 256), (1, 4)), -0.2, 0.2), 0.25, 2.0),
        "spread": jnp.clip(jnp.exp(jax.random.uniform(key_list[4], (FIELDS, LEVELS), jnp.float32, math.log(0.02), math.log(0.2))), 0.02, 0.2),
        "mixing": jnp.clip(jnp.exp(jax.random.uniform(key_list[5], (LEVELS,), jnp.float32, math.log(0.02), math.log(0.2))), 0.02, 0.2),
        "thickness": jnp.clip(jnp.exp(jax.random.uniform(key_list[6], (LEVELS,), jnp.float32, math.log(0.5), math.log(2.0))), 0.5, 2.0),
    }


OPPOSITE = np.array([1, 0, 3, 2], np.int32)


def rim_rows(values, width):
    west_rim = values[..., ::width]
    east_rim = values[..., width - 1::width]
    south_rim = values[..., :width]
    north_rim = values[..., -width:]
    return jnp.concatenate([west_rim, east_rim, south_rim, north_rim], axis=-1)


def beside_values(values, rims, width):
    cells_total = values.shape[-1]
    leading = values.shape[:-1]
    places = jnp.arange(cells_total, dtype=jnp.int32)
    column_index = places % width
    row_index = places // width
    west_full = jnp.broadcast_to(rims[..., 0, :, None], leading + (width, width)).reshape(leading + (cells_total,))
    east_full = jnp.broadcast_to(rims[..., 1, :, None], leading + (width, width)).reshape(leading + (cells_total,))
    south_full = jnp.broadcast_to(rims[..., 2, None, :], leading + (width, width)).reshape(leading + (cells_total,))
    north_full = jnp.broadcast_to(rims[..., 3, None, :], leading + (width, width)).reshape(leading + (cells_total,))
    zero_cell = jnp.zeros(leading + (1,), jnp.float32)
    zero_line = jnp.zeros(leading + (width,), jnp.float32)
    west_side = jnp.where(column_index == 0, west_full, jnp.concatenate([zero_cell, values[..., :-1]], -1))
    east_side = jnp.where(column_index == width - 1, east_full, jnp.concatenate([values[..., 1:], zero_cell], -1))
    south_side = jnp.where(row_index == 0, south_full, jnp.concatenate([zero_line, values[..., :-width]], -1))
    north_side = jnp.where(row_index == width - 1, north_full, jnp.concatenate([values[..., width:], zero_line], -1))
    return west_side, east_side, south_side, north_side


def orient(picked, links, vector):
    code = links[..., 3]
    partner = links[..., 2]
    lead = code.ndim
    extra = picked.ndim - lead
    tail_shape = code.shape + (1,) * extra
    flipped = jnp.where((code != 0).reshape(tail_shape), jnp.flip(picked, -1), picked)
    flipped = flipped * (partner >= 0).astype(jnp.float32).reshape(tail_shape)
    if vector:
        turn_shape = code.shape + (1,) * (extra - 1)
        cosine_part = ((code == 0).astype(jnp.float32) - (code == 2).astype(jnp.float32)).reshape(turn_shape)
        sine_part = ((code == 1).astype(jnp.float32) - (code == 3).astype(jnp.float32)).reshape(turn_shape)
        eastward = jnp.take(flipped, 0, axis=lead)
        northward = jnp.take(flipped, 1, axis=lead)
        scalar_part = jnp.take(flipped, 2, axis=lead)
        flipped = jnp.stack([cosine_part * eastward + sine_part * northward,
                             cosine_part * northward - sine_part * eastward, scalar_part], axis=lead)
    return jnp.moveaxis(flipped, lead - 1, -2)


def slab_step(fields, wet, rims, spread, mixing, thickness, width):
    wet_cells = wet[..., None, None, :]
    masked = fields * wet_cells
    west_side, east_side, south_side, north_side = beside_values(masked, rims, width)
    flat_term = west_side + east_side + south_side + north_side - 4.0 * masked
    above = jnp.concatenate([masked[..., 1:, :], masked[..., -1:, :]], axis=-2)
    below = jnp.concatenate([masked[..., :1, :], masked[..., :-1, :]], axis=-2)
    column_term = above + below - 2.0 * masked
    updated = wet_cells * (masked + spread[:, :, None] * flat_term + mixing[:, None] * column_term)
    flux = 0.5 * (east_side[..., 0, :, :] - west_side[..., 0, :, :] + north_side[..., 1, :, :] - south_side[..., 1, :, :])
    source = wet * jnp.sum(thickness[:, None] * flux, axis=-2)
    return updated, source


def surface_apply(values, wet, rims, diagonal, width):
    west_side, east_side, south_side, north_side = beside_values(values, rims, width)
    return wet * ((4.0 + diagonal) * values - (west_side + east_side + south_side + north_side))


def pick_global(packs, links):
    group_shift = links[..., 0]
    strip_shift = links[..., 1]
    partner = jnp.maximum(links[..., 2], 0)
    group_index = (jnp.arange(TILE_GROUPS, dtype=jnp.int32)[:, None, None, None] + group_shift) % TILE_GROUPS
    strip_index = (jnp.arange(STRIP_GROUPS, dtype=jnp.int32)[None, :, None, None] + strip_shift) % STRIP_GROUPS
    opposite = jnp.broadcast_to(jnp.asarray(OPPOSITE)[None, None, None, :], partner.shape)
    return packs[group_index, strip_index, partner, ..., opposite, :]


def reference(fields, wet_land, links, surface_diagonal, spread, mixing, thickness):
    wet = wet_land.astype(jnp.float32)
    masked = fields * wet[:, :, :, None, None, :]
    slab_packs = rim_rows(masked, TILE).reshape(masked.shape[:-1] + (4, TILE))
    slab_rims = orient(pick_global(slab_packs, links), links, True)

    def one_group(items):
        group_fields, group_wet, group_rims = items
        return slab_step(group_fields, group_wet, group_rims, spread, mixing, thickness, TILE)

    updated, source = lax.map(one_group, (fields, wet, slab_rims))

    def surface_image(values):
        packs = rim_rows(values, TILE).reshape(values.shape[:-1] + (4, TILE))
        rims = orient(pick_global(packs, links), links, False)
        return surface_apply(values, wet, rims, surface_diagonal, TILE)

    solution = jnp.zeros_like(source)
    residual = source
    direction = source
    norm_now = jnp.sum(residual * residual)
    for iteration in range(ITERS):
        image = surface_image(direction)
        alpha = norm_now / jnp.sum(direction * image)
        solution = solution + alpha * direction
        residual = residual - alpha * image
        if iteration + 1 < ITERS:
            norm_next = jnp.sum(residual * residual)
            direction = residual + (norm_next / norm_now) * direction
            norm_now = norm_next
    return updated, solution, residual
```

```python
import functools

import jax
import jax.numpy as jnp
from jax import lax
from jax.experimental import pallas as pl
from jax.experimental.pallas import tpu as pltpu
from jax.sharding import PartitionSpec as P

TILE = 90
SLOTS = 3
FIELDS = 3
LEVELS = 4
CELLS = TILE * TILE
LANES = 128
BLOCKS = 64
WIDE = LANES * BLOCKS
SPLIT = 45
CENTRE = 5.0
MESH = pl.DeviceIdType.MESH
WEST, EAST, SOUTH, NORTH = 0, 1, 2, 3


def take_lanes(rows, index):
    return jnp.take_along_axis(rows, index, axis=1, mode="promise_in_bounds")


def block(k):
    return slice(k * LANES, (k + 1) * LANES)


def beside(x, not_west, not_east):
    west = pltpu.roll(x, 1, 1) * not_west
    east = pltpu.roll(x, WIDE - 1, 1) * not_east
    south = pltpu.roll(x, TILE, 1)
    north = pltpu.roll(x, WIDE - TILE, 1)
    return west, east, south, north


def lane_row(shape=(4, LANES)):
    return lax.broadcasted_iota(jnp.int32, shape, 1)


def rims_of(load, rim):
    def merged(first, last):
        values = [(load(k), rim(k)) for k in range(first, last)]
        chains = []
        for start in range(4):
            total = None
            for value, mask in values[start::4]:
                kept = value * mask
                total = kept if total is None else total + kept
            chains.append(total)
        return (chains[0] + chains[1]) + (chains[2] + chains[3])

    low = merged(0, SPLIT)
    high = merged(SPLIT, BLOCKS)
    lane = lane_row()
    west_lane = (lane * TILE) & (LANES - 1)
    east_lane = (lane * TILE + (TILE - 1)) & (LANES - 1)
    west = jnp.where(lane < 64, take_lanes(low, west_lane), take_lanes(high, west_lane))
    east = jnp.where(lane < 64, take_lanes(low, east_lane), take_lanes(high, east_lane))
    south = load(0)
    north = jnp.where(lane < 54, pltpu.roll(load(62), 54, 1), pltpu.roll(load(63), 54, 1))
    return west, east, south, north


def spread_rims(west, east, south, north):
    lane = lane_row()
    half = lax.shift_right_logical(lane, 1)
    odd = (lane & 1) == 1
    west_row = (half * 37) & 63
    east_row = (lax.shift_right_logical(lane + 39, 1) * 37) & 63
    low = jnp.where(odd, take_lanes(east, east_row), take_lanes(west, west_row))
    high = jnp.where(odd, take_lanes(east, east_row + 64), take_lanes(west, west_row + 64))
    first = jnp.where(lane < TILE, south, 0.0)
    turned = pltpu.roll(north, 74, 1)
    before = jnp.where(lane >= 74, turned, 0.0)
    final = jnp.where(lane < 36, turned, 0.0)
    columns = jnp.concatenate([low] * SPLIT + [high] * (BLOCKS - SPLIT), axis=1)
    return columns, first, before, final


def flip(rows, flags):
    back = (TILE - 1 - lane_row()) & (LANES - 1)
    return jnp.where(flags > 0.0, take_lanes(rows, back), rows)


def kernel(
    sizes,
    links, spread, mixing, thickness, fields, wet_land, diagonal,
    adjoint, answer, remainder,
    raw, raw_wet, raw_diagonal, masked, stepped, wet, wet_levels, centre_term,
    not_west, not_east, rim_mask, east_flow, north_flow, first_field, second_field, third_field,
    flags, turn_a, turn_b, valid, spreads, mixings, weights,
    rows_a, rows_b, slab_rows, answer_rows, remainder_rows,
    send_1, recv_1, send_2, recv_2, send_3, recv_3, send_slab, recv_slab,
    plane, column,
    in_sems, out_sem, send_sems, recv_sems, hello,
):
    groups, strips, length = sizes
    t = lax.axis_index("tiles")
    s = lax.axis_index("strip")
    core = lax.rem(t, 2)
    chip = lax.div(t, 2)
    z = lax.rem(chip, length)
    x = lax.div(chip, length)
    planes = groups // length * strips
    here = (x * strips + s) * 2 + core

    def beside_device(dt, ds):
        return (lax.rem(t + dt + groups, groups), lax.rem(s + ds + strips, strips))

    def plane_device(offset):
        other = lax.rem(here + offset, planes)
        at_x = lax.div(other, 2 * strips)
        at_s = lax.rem(lax.div(other, 2), strips)
        return ((at_x * length + z) * 2 + lax.rem(other, 2), at_s)

    def column_device(offset):
        return ((x * length + lax.rem(z + offset + length, length)) * 2 + core, s)

    reach = min(4, length // 2)
    near = [(dt, ds) for dt in (-1, 0, 1) for ds in (-1, 0, 1) if (dt, ds) != (0, 0)]
    along = []
    for d in range(1, reach + 1):
        along += [d] if 2 * d == length else [d, -d]
    barrier = pltpu.get_barrier_semaphore()
    for dt, ds in near:
        pl.semaphore_signal(barrier, inc=1, device_id=beside_device(dt, ds), device_id_type=MESH)
    for offset in along:
        pl.semaphore_signal(barrier, inc=1, device_id=column_device(offset), device_id_type=MESH)
    for offset in range(1, planes):
        pl.semaphore_signal(barrier, inc=1, device_id=plane_device(offset), device_id_type=MESH)

    wet_copy = pltpu.make_async_copy(wet_land, raw_wet, in_sems.at[9])
    wet_copy.start()
    field_copies = {}
    for f in (0, 1, 2):
        for k in range(SLOTS):
            a = k * FIELDS + f
            field_copies[a] = pltpu.make_async_copy(fields.at[a], raw.at[a], in_sems.at[a])
            field_copies[a].start()
    diagonal_copy = pltpu.make_async_copy(diagonal, raw_diagonal, in_sems.at[10])
    diagonal_copy.start()

    cell = lax.broadcasted_iota(jnp.int32, (4, WIDE), 1)
    row = lax.shift_right_logical(cell * 11651, 20)
    place = cell - row * TILE
    not_west[...] = jnp.where(place == 0, 0.0, 1.0)
    not_east[...] = jnp.where(place == TILE - 1, 0.0, 1.0)
    at_rim = (place == 0) | (place == TILE - 1)
    rim_mask[...] = jnp.where(at_rim & (cell < CELLS), 1.0, 0.0)
    zero_row = jnp.zeros((1, LANES), jnp.float32)
    for side in range(4):
        for k in range(SLOTS):
            code = links[k, side, 3]
            there = (links[k, side, 2] >= 0).astype(jnp.float32)
            one = lambda flag: flag.astype(jnp.float32)
            fill = lambda value: jnp.full((1, LANES), value, jnp.float32)
            flags[side, k : k + 1, :] = fill(one(code != 0))
            valid[side, k : k + 1, :] = fill(there)
            turn_a[side, k : k + 1, :] = fill(there * (one(code == 0) - one(code == 2)))
            turn_b[side, k : k + 1, :] = fill(there * (one(code == 1) - one(code == 3)))
        for table in (flags, valid, turn_a, turn_b, rows_a, rows_b):
            table[side, 3:4, :] = zero_row
    for l in range(LEVELS):
        weights[l : l + 1, :] = jnp.full((1, LANES), thickness[l], jnp.float32)
        mixings[l : l + 1, :] = jnp.full((1, LANES), mixing[l], jnp.float32)
        for f in range(FIELDS):
            spreads[f, l : l + 1, :] = jnp.full((1, LANES), spread[f, l], jnp.float32)
    for table in (wet, centre_term, east_flow, north_flow):
        table[...] = jnp.zeros((4, WIDE), jnp.float32)
    tail = jnp.zeros((4, LANES), jnp.float32)
    for a in range(SLOTS * FIELDS):
        masked[a, :, block(63)] = tail

    def tiled(rows):
        return jnp.concatenate([rows] * BLOCKS, axis=1)

    wet_copy.wait()
    wet[0:3, 0:CELLS] = raw_wet[...].astype(jnp.float32)
    for k in range(SLOTS):
        wet_levels[k] = jnp.broadcast_to(wet[k : k + 1, :], (4, WIDE))

    def mask_field(a, k):
        kept = wet_levels[k, :, 0:CELLS] > 0.0
        masked[a, :, 0:CELLS] = jnp.where(kept, raw[a], 0.0)

    for k in range(SLOTS):
        for f, flow in ((0, east_flow), (1, north_flow)):
            a = k * FIELDS + f
            field_copies[a].wait()
            mask_field(a, k)
            scaled = masked[a] * tiled(weights[...])
            flow[k : k + 1, :] = jnp.sum(scaled, axis=0, keepdims=True)

    rim = lambda k: rim_mask[:, block(k)]
    for part, flow in ((0, east_flow), (1, north_flow)):
        for side, value in enumerate(rims_of(lambda k: flow[:, block(k)], rim)):
            for k in range(SLOTS):
                send_1[side, k, part : part + 1, :] = value[k : k + 1, :]

    pl.semaphore_wait(barrier, len(near) + len(along) + planes - 1)

    def exchange(sent, received, slot, width):
        for d in (-1, 0, 1):
            for side, device in (
                (EAST, beside_device(1, d)),
                (WEST, beside_device(-1, d)),
                (NORTH, beside_device(d, 1)),
                (SOUTH, beside_device(d, -1)),
            ):
                pltpu.make_async_remote_copy(
                    src_ref=sent.at[side],
                    dst_ref=received.at[side ^ 1, pl.ds((1 - d) * width, width)],
                    send_sem=send_sems.at[slot],
                    recv_sem=recv_sems.at[slot],
                    device_id=device,
                    device_id_type=MESH,
                ).start()

    def whole(buffer, slot):
        return pltpu.make_async_remote_copy(
            src_ref=buffer,
            dst_ref=buffer,
            send_sem=send_sems.at[slot],
            recv_sem=recv_sems.at[slot],
            device_id=beside_device(1, 0),
            device_id_type=MESH,
        )

    def source_of(k, side):
        step = links[k, side, 1] if side in (WEST, EAST) else links[k, side, 0]
        step = jnp.clip(step, -1, 1) + 1
        return step * SLOTS + jnp.clip(links[k, side, 2], 0, SLOTS - 1)

    exchange(send_1, recv_1, 0, SLOTS)
    greeting = reach
    rounds = []
    while greeting < length // 2:
        rounds.append(greeting)
        greeting *= 2

    def greet(i):
        if i < len(rounds):
            for offset in (rounds[i], -rounds[i]):
                pl.semaphore_signal(
                    hello.at[i], inc=1, device_id=column_device(offset), device_id_type=MESH
                )

    def greeted(i):
        if i < len(rounds):
            pl.semaphore_wait(hello.at[i], 2)

    greet(0)

    for k in range(SLOTS):
        field_copies[k * FIELDS + 2].wait()
        mask_field(k * FIELDS + 2, k)

    def slab_rims(a, carry):
        for side, value in enumerate(rims_of(lambda k: masked[a, :, block(k)], rim)):
            send_slab[side, a] = value
        return carry

    lax.fori_loop(0, SLOTS * FIELDS, slab_rims, 0)
    exchange(send_slab, recv_slab, 3, SLOTS * FIELDS)

    def flux_inside():
        west, east, _, _ = beside(east_flow[...], not_west[...], not_east[...])
        _, _, south, north = beside(north_flow[...], not_west[...], not_east[...])
        return 0.5 * wet[...] * (east - west + north - south)

    first_field[...] = flux_inside()
    diagonal_copy.wait()
    centre_term[0:3, 0:CELLS] = raw_diagonal[...] + (4.0 - CENTRE)

    def add_rims(target, scale, west, east, south, north):
        columns, first, before, final = spread_rims(west, east, south, north)
        target[...] += scale * wet[...] * (columns * rim_mask[...])
        for k, value in ((0, first), (62, before), (63, final)):
            target[:, block(k)] += scale * wet[:, block(k)] * value

    def operator_inside(target, values):
        west, east, south, north = beside(values[...], not_west[...], not_east[...])
        target[...] = wet[...] * (
            centre_term[...] * values[...] - ((west + east) + (south + north))
        )

    def send_surface(values, sent, received, slot):
        for side, value in enumerate(rims_of(lambda k: values[:, block(k)], rim)):
            for k in range(SLOTS):
                sent[side, k] = value[k : k + 1, :]
        exchange(sent, received, slot, SLOTS)

    def received_surface(received, slot):
        whole(received, slot).wait_recv()
        out = []
        for side in range(4):
            for k in range(SLOTS):
                rows_a[side, k : k + 1, :] = received[side, source_of(k, side)]
            out.append(flip(rows_a[side] * valid[side], flags[side]))
        return out

    whole(recv_1, 0).wait_recv()
    gathered = []
    for side in range(4):
        for k in range(SLOTS):
            pair = recv_1[side, source_of(k, side)]
            rows_a[side, k : k + 1, :] = pair[0:1, :]
            rows_b[side, k : k + 1, :] = pair[1:2, :]
        a, b = turn_a[side], turn_b[side]
        if side in (WEST, EAST):
            turned = a * rows_a[side] + b * rows_b[side]
        else:
            turned = a * rows_b[side] - b * rows_a[side]
        if side in (WEST, SOUTH):
            turned = -turned
        gathered.append(flip(turned, flags[side]))
    add_rims(first_field, 0.5, *gathered)
    send_surface(first_field, send_2, recv_2, 1)

    operator_inside(second_field, first_field)
    add_rims(second_field, -1.0, *received_surface(recv_2, 1))
    send_surface(second_field, send_3, recv_3, 2)
    greeted(0)
    greet(1)

    operator_inside(third_field, second_field)

    def total(value):
        return jnp.sum(jnp.sum(value, axis=1, keepdims=True), axis=0, keepdims=True)

    moment_0 = total(first_field[...] * first_field[...])
    moment_1 = total(first_field[...] * second_field[...])
    moment_2 = total(second_field[...] * second_field[...])
    add_rims(third_field, -1.0, *received_surface(recv_3, 2))
    moment_3 = total(second_field[...] * third_field[...])
    lane = lane_row((1, LANES))
    packed = jnp.where(lane == 0, moment_0, 0.0)
    packed = jnp.where(lane == 1, moment_1, packed)
    packed = jnp.where(lane == 2, moment_2, packed)
    packed = jnp.where(lane == 3, moment_3, packed)

    def share(buffer, position, value, devices, slot):
        buffer[position] = value
        for device in devices:
            pltpu.make_async_remote_copy(
                src_ref=buffer.at[position],
                dst_ref=buffer.at[position],
                send_sem=send_sems.at[slot],
                recv_sem=recv_sems.at[slot],
                device_id=device,
                device_id_type=MESH,
            ).start()

    def shared(buffer, count, slot):
        return whole(buffer.at[pl.ds(0, count)], slot)

    share(plane, here, packed, [plane_device(o) for o in range(1, planes)], 4)
    for i in range(1, len(rounds)):
        greeted(i)
        greet(i + 1)
    shared(plane, planes - 1, 4).wait_recv()
    packed = jnp.sum(plane[...], axis=0)
    offsets = []
    for d in range(length // 2, 0, -1):
        offsets += [d] if 2 * d == length else [d, -d]
    share(column, z, packed, [column_device(o) for o in offsets], 5)

    whole(recv_slab, 3).wait_recv()

    def slab_orient(k, carry):
        for side in range(4):
            code = links[k, side, 3]
            there = (links[k, side, 2] >= 0).astype(jnp.float32)
            cosine = there * ((code == 0).astype(jnp.float32) - (code == 2).astype(jnp.float32))
            sine = there * ((code == 1).astype(jnp.float32) - (code == 3).astype(jnp.float32))
            turn = (code != 0).astype(jnp.float32)
            at = source_of(k, side) * FIELDS
            u, v, scalar = (recv_slab[side, at + f] for f in range(FIELDS))
            values = (cosine * u + sine * v, cosine * v - sine * u, there * scalar)
            for f in range(FIELDS):
                slab_rows[side, k * FIELDS + f] = flip(
                    values[f], jnp.full((4, LANES), turn, jnp.float32)
                )
        return carry

    lax.fori_loop(0, SLOTS, slab_orient, 0)

    def slab_step(a, carry):
        k = lax.div(a, FIELDS)
        f = lax.rem(a, FIELDS)
        m = masked[a]
        west, east, south, north = beside(m, not_west[...], not_east[...])
        columns, first, before, final = spread_rims(*(slab_rows[side, a] for side in range(4)))
        flat = (west + east) + (south + north) + columns * rim_mask[...]
        flat = jnp.concatenate(
            [
                flat[:, block(0)] + first,
                flat[:, LANES : 62 * LANES],
                flat[:, block(62)] + before,
                flat[:, block(63)] + final,
            ],
            axis=1,
        )
        flat = flat - 4.0 * m
        above = jnp.concatenate([m[1:4], m[3:4]], axis=0)
        below = jnp.concatenate([m[0:1], m[0:3]], axis=0)
        vertical = above + below - 2.0 * m
        updated = wet_levels[k] * (
            m + tiled(spreads[f]) * flat + tiled(mixings[...]) * vertical
        )
        stepped[a] = updated[:, 0:CELLS]
        pltpu.make_async_copy(stepped.at[a], adjoint.at[a], out_sem.at[0]).start()
        return carry

    lax.fori_loop(0, SLOTS * FIELDS, slab_step, 0)

    shared(column, length - 1, 5).wait_recv()
    packed = jnp.sum(column[...], axis=0)
    n0, n1, n2, n3 = (
        jnp.sum(jnp.where(lane == i, packed, 0.0), axis=1, keepdims=True) for i in range(4)
    )
    r1, r2, r3 = n1 / n0, n2 / n0, n3 / n0
    mu = r1 + CENTRE
    alpha_0 = 1.0 / mu
    beta = (r2 - r1 * r1) * alpha_0 * alpha_0
    applied = (r1 * r1 * r1 - 2.0 * r1 * r2 + r3) * alpha_0 * alpha_0 + CENTRE * beta
    alpha_1 = beta / (applied - beta * beta * mu)
    c1 = alpha_0 + alpha_1 * (1.0 + beta)
    c2 = alpha_0 * alpha_1
    r, v, w = first_field[...], second_field[...], third_field[...]
    found = (c1 - CENTRE * c2) * r - c2 * v
    left = (1.0 - CENTRE * c1 + CENTRE * CENTRE * c2) * r + (2.0 * CENTRE * c2 - c1) * v + c2 * w
    answer_rows[...] = found[0:3, 0:CELLS]
    remainder_rows[...] = left[0:3, 0:CELLS]
    answer_copy = pltpu.make_async_copy(answer_rows, answer, out_sem.at[1])
    remainder_copy = pltpu.make_async_copy(remainder_rows, remainder, out_sem.at[2])
    answer_copy.start()
    remainder_copy.start()
    for slot, buffer in enumerate((recv_1, recv_2, recv_3, recv_slab)):
        whole(buffer, slot).wait_send()
    shared(plane, planes - 1, 4).wait_send()
    shared(column, length - 1, 5).wait_send()
    pltpu.make_async_copy(stepped, adjoint, out_sem.at[0]).wait()
    answer_copy.wait()
    remainder_copy.wait()


def make(mesh, length):
    groups, strips = mesh.shape["tiles"], mesh.shape["strip"]
    planes = groups // length * strips
    slabs = SLOTS * FIELDS
    f32 = jnp.float32
    V = lambda *shape: pltpu.VMEM(shape, f32)
    smem = pl.BlockSpec(memory_space=pltpu.SMEM)
    hbm = pl.BlockSpec(memory_space=pl.ANY)
    call = pl.pallas_call(
        functools.partial(kernel, (groups, strips, length)),
        out_shape=(
            jax.ShapeDtypeStruct((slabs, LEVELS, CELLS), f32),
            jax.ShapeDtypeStruct((SLOTS, CELLS), f32),
            jax.ShapeDtypeStruct((SLOTS, CELLS), f32),
        ),
        in_specs=[smem] * 4 + [hbm] * 3,
        out_specs=(hbm, hbm, hbm),
        scratch_shapes=[
            V(slabs, LEVELS, CELLS),
            pltpu.VMEM((SLOTS, CELLS), jnp.int32),
            V(SLOTS, CELLS),
            V(slabs, LEVELS, WIDE),
            V(slabs, LEVELS, CELLS),
            V(4, WIDE),
            V(SLOTS, 4, WIDE),
            V(4, WIDE),
            V(4, WIDE), V(4, WIDE), V(4, WIDE),
            V(4, WIDE), V(4, WIDE), V(4, WIDE), V(4, WIDE), V(4, WIDE),
            V(4, 4, LANES), V(4, 4, LANES), V(4, 4, LANES), V(4, 4, LANES),
            V(FIELDS, 4, LANES), V(4, LANES), V(4, LANES),
            V(4, 4, LANES), V(4, 4, LANES), V(4, slabs, 4, LANES),
            V(SLOTS, CELLS), V(SLOTS, CELLS),
            V(4, SLOTS, 2, LANES), V(4, 3 * SLOTS, 2, LANES),
            V(4, SLOTS, 1, LANES), V(4, 3 * SLOTS, 1, LANES),
            V(4, SLOTS, 1, LANES), V(4, 3 * SLOTS, 1, LANES),
            V(4, slabs, 4, LANES), V(4, 3 * slabs, 4, LANES),
            V(planes, 1, LANES), V(length, 1, LANES),
            pltpu.SemaphoreType.DMA((11,)),
            pltpu.SemaphoreType.DMA((3,)),
            pltpu.SemaphoreType.DMA((6,)),
            pltpu.SemaphoreType.DMA((6,)),
            pltpu.SemaphoreType.REGULAR((4,)),
        ],
        compiler_params=pltpu.CompilerParams(
            collective_id=0, has_side_effects=True, vmem_limit_bytes=24 * 1024 * 1024
        ),
        name="slab_and_gradients",
    )

    def on_device(fields, wet_land, links, surface_diagonal, spread, mixing, thickness):
        updated, found, left = call(
            links[0, 0],
            spread,
            mixing,
            thickness,
            fields.reshape(slabs, LEVELS, CELLS),
            wet_land.reshape(SLOTS, CELLS),
            surface_diagonal.reshape(SLOTS, CELLS),
        )
        return updated.reshape(fields.shape), found[None, None], left[None, None]

    return jax.shard_map(
        on_device,
        mesh=mesh,
        in_specs=(
            P("tiles", "strip", None, None, None, None),
            P("tiles", "strip", None, None),
            P("tiles", "strip", None, None, None),
            P("tiles", "strip", None, None),
            P(),
            P(),
            P(),
        ),
        out_specs=(
            P("tiles", "strip", None, None, None, None),
            P("tiles", "strip", None, None),
            P("tiles", "strip", None, None),
        ),
        check_vma=False,
    )


def solution(mesh):
    return make(mesh, 32)
```

```python
import functools

import jax
import jax.numpy as jnp
from jax import lax
from jax.experimental import pallas as pl
from jax.experimental.pallas import tpu as pltpu
from jax.sharding import PartitionSpec as P

TILE = 90
SLOTS = 3
FIELDS = 3
LEVELS = 4
CELLS = TILE * TILE
LANES = 128
BLOCKS = 64
WIDE = LANES * BLOCKS
SPLIT = 45
CENTRE = 5.0
GRANT = 57_000_000
MESH = pl.DeviceIdType.MESH
WEST, EAST, SOUTH, NORTH = 0, 1, 2, 3


def take_lanes(rows, index):
    return jnp.take_along_axis(rows, index, axis=1, mode="promise_in_bounds")


def block(k):
    return slice(k * LANES, (k + 1) * LANES)


def beside(x, not_west, not_east):
    west = pltpu.roll(x, 1, 1) * not_west
    east = pltpu.roll(x, WIDE - 1, 1) * not_east
    south = pltpu.roll(x, TILE, 1)
    north = pltpu.roll(x, WIDE - TILE, 1)
    return west, east, south, north


def lane_row(shape=(4, LANES)):
    return lax.broadcasted_iota(jnp.int32, shape, 1)


def rims_of(load, rim):
    def merged(first, last):
        values = [(load(k), rim(k)) for k in range(first, last)]
        chains = []
        for start in range(4):
            total = None
            for value, mask in values[start::4]:
                kept = value * mask
                total = kept if total is None else total + kept
            chains.append(total)
        return (chains[0] + chains[1]) + (chains[2] + chains[3])

    low = merged(0, SPLIT)
    high = merged(SPLIT, BLOCKS)
    lane = lane_row()
    west_lane = (lane * TILE) & (LANES - 1)
    east_lane = (lane * TILE + (TILE - 1)) & (LANES - 1)
    west = jnp.where(lane < 64, take_lanes(low, west_lane), take_lanes(high, west_lane))
    east = jnp.where(lane < 64, take_lanes(low, east_lane), take_lanes(high, east_lane))
    south = load(0)
    north = jnp.where(lane < 54, pltpu.roll(load(62), 54, 1), pltpu.roll(load(63), 54, 1))
    return west, east, south, north


def spread_rims(west, east, south, north):
    lane = lane_row()
    half = lax.shift_right_logical(lane, 1)
    odd = (lane & 1) == 1
    west_row = (half * 37) & 63
    east_row = (lax.shift_right_logical(lane + 39, 1) * 37) & 63
    low = jnp.where(odd, take_lanes(east, east_row), take_lanes(west, west_row))
    high = jnp.where(odd, take_lanes(east, east_row + 64), take_lanes(west, west_row + 64))
    first = jnp.where(lane < TILE, south, 0.0)
    turned = pltpu.roll(north, 74, 1)
    before = jnp.where(lane >= 74, turned, 0.0)
    final = jnp.where(lane < 36, turned, 0.0)
    columns = jnp.concatenate([low] * SPLIT + [high] * (BLOCKS - SPLIT), axis=1)
    return columns, first, before, final


def flip(rows, flags):
    back = (TILE - 1 - lane_row()) & (LANES - 1)
    return jnp.where(flags > 0.0, take_lanes(rows, back), rows)


def kernel(
    sizes,
    links_in, spread_in, mixing_in, thickness_in, fields, wet_land, diagonal,
    adjoint, vectors, scales,
    raw, raw_wet, raw_diagonal, masked, stepped, vector_rows, scale_row, wet, wet_levels, centre_term,
    not_west, not_east, rim_mask, east_flow, north_flow,
    flags, turn_a, turn_b, valid, spreads, mixings, weights,
    rows_a, rows_b, slab_rows,
    send_1, recv_1, send_2, recv_2, send_3, recv_3, send_slab, recv_slab,
    plane, column, links, spread, mixing, thickness,
    in_sems, out_sems, send_sems, recv_sems, hello,
):
    groups, strips, length = sizes
    wet_copy = pltpu.make_async_copy(wet_land, raw_wet, in_sems.at[9])
    wet_copy.start()
    def field_copy(a):
        return pltpu.make_async_copy(fields.at[a], raw.at[a], in_sems.at[a])

    for k in range(SLOTS):
        for f in range(2):
            field_copy(k * FIELDS + f).start()
    diagonal_copy = pltpu.make_async_copy(diagonal, raw_diagonal, in_sems.at[10])
    diagonal_copy.start()
    table_copies = [
        pltpu.make_async_copy(source, target, in_sems.at[11 + i])
        for i, (source, target) in enumerate(
            (
                (links_in, links),
                (spread_in, spread),
                (mixing_in, mixing),
                (thickness_in, thickness),
            )
        )
    ]
    for copy in table_copies:
        copy.start()
    for k in range(SLOTS):
        field_copy(k * FIELDS + 2).start()

    t = lax.axis_index("tiles")
    s = lax.axis_index("strip")
    core = lax.rem(t, 2)
    chip = lax.div(t, 2)
    z = lax.rem(chip, length)
    x = lax.div(chip, length)
    planes = groups // length * strips
    here = (x * strips + s) * 2 + core

    def beside_device(dt, ds):
        return (lax.rem(t + dt + groups, groups), lax.rem(s + ds + strips, strips))

    def plane_device(offset):
        other = lax.rem(here + offset, planes)
        at_x = lax.div(other, 2 * strips)
        at_s = lax.rem(lax.div(other, 2), strips)
        return ((at_x * length + z) * 2 + lax.rem(other, 2), at_s)

    def column_device(offset):
        return ((x * length + lax.rem(z + offset + length, length)) * 2 + core, s)

    near = [(dt, ds) for dt in (-1, 0, 1) for ds in (-1, 0, 1) if (dt, ds) != (0, 0)]
    stride = 2 * length

    def offset_device(dx, ds, dz, other):
        along_x = lax.rem(x + dx + groups // stride, groups // stride)
        along_z = lax.rem(z + dz + length, length)
        along_s = lax.rem(s + ds + strips, strips)
        return ((along_x * length + along_z) * 2 + (1 - core if other else core), along_s)

    first = [(1, 0, 0, 0), (-1, 0, 0, 0), (0, 0, 1, 0), (0, 0, -1, 0)]
    barrier = pltpu.get_barrier_semaphore()
    for dt, ds in near:
        pl.semaphore_signal(barrier, inc=1, device_id=beside_device(dt, ds), device_id_type=MESH)
    for offset in first:
        pl.semaphore_signal(
            barrier, inc=1, device_id=offset_device(*offset), device_id_type=MESH
        )

    rounds = [
        first + [(0, 1, 0, 0), (0, -1, 0, 0), (0, 0, 0, 1), (0, 1, 0, 1), (0, -1, 0, 1)],
        [(2, 0, 0, 0), (0, 2, 0, 0), (0, 0, 0, 1), (0, 0, 2, 0), (0, 0, -2, 0)],
    ]
    reach = 4
    while reach < length // 2:
        rounds.append([(0, 0, reach, 0), (0, 0, -reach, 0)])
        reach *= 2

    def greet(i):
        if i < len(rounds):
            for offset in rounds[i]:
                pl.semaphore_signal(
                    hello.at[i], inc=1, device_id=offset_device(*offset), device_id_type=MESH
                )

    def greeted(i):
        if i < len(rounds):
            pl.semaphore_wait(hello.at[i], len(rounds[i]))

    cell = lax.broadcasted_iota(jnp.int32, (4, WIDE), 1)
    row = lax.shift_right_logical(cell * 11651, 20)
    place = cell - row * TILE
    at_rim = (place == 0) | (place == TILE - 1)
    rim_mask[...] = jnp.where(at_rim & (cell < CELLS), 1.0, 0.0)
    tail = jnp.zeros((4, LANES), jnp.float32)
    wet[:, block(63)] = tail
    wet[3:4, :] = jnp.zeros((1, WIDE), jnp.float32)
    for a in range(SLOTS * FIELDS):
        masked[a, :, block(63)] = tail

    def tiled(rows):
        return jnp.concatenate([rows] * BLOCKS, axis=1)

    for copy in table_copies:
        copy.wait()
    for l in range(LEVELS):
        weights[l : l + 1, :] = jnp.full((1, LANES), thickness[l], jnp.float32)
    wet_copy.wait()
    for k in range(SLOTS):
        wet[k : k + 1, 0:CELLS] = raw_wet[k].astype(jnp.float32)
        wet_levels[k] = jnp.broadcast_to(wet[k : k + 1, :], (4, WIDE))

    rim = lambda k: rim_mask[:, block(k)]

    def slab_rims(k, f):
        a = k * FIELDS + f
        field_copy(a).wait()
        kept = wet_levels[k, :, 0:CELLS] > 0.0
        masked[a, :, 0:CELLS] = jnp.where(kept, raw[a], 0.0)
        values = rims_of(lambda i: masked[a, :, block(i)], rim)
        for side, value in enumerate(values):
            send_slab[side, a] = value
        return values

    def velocity_rims(i, carry):
        k = lax.div(i, 2)
        f = lax.rem(i, 2)
        for side, value in enumerate(slab_rims(k, f)):
            send_1[side, i] = jnp.sum(value * weights[...], axis=0, keepdims=True)
        return carry

    lax.fori_loop(0, 2 * SLOTS, velocity_rims, 0)

    pl.semaphore_wait(barrier, len(near) + len(first))

    def exchange(sent, received, slot, width):
        for d in (-1, 0, 1):
            for side, device in (
                (EAST, beside_device(1, d)),
                (WEST, beside_device(-1, d)),
                (NORTH, beside_device(d, 1)),
                (SOUTH, beside_device(d, -1)),
            ):
                pltpu.make_async_remote_copy(
                    src_ref=sent.at[side],
                    dst_ref=received.at[side ^ 1, pl.ds((1 - d) * width, width)],
                    send_sem=send_sems.at[slot],
                    recv_sem=recv_sems.at[slot],
                    device_id=device,
                    device_id_type=MESH,
                ).start()

    def whole(buffer, slot):
        return pltpu.make_async_remote_copy(
            src_ref=buffer,
            dst_ref=buffer,
            send_sem=send_sems.at[slot],
            recv_sem=recv_sems.at[slot],
            device_id=beside_device(1, 0),
            device_id_type=MESH,
        )

    def source_of(k, side):
        step = links[k, side, 1] if side in (WEST, EAST) else links[k, side, 0]
        step = jnp.clip(step, -1, 1) + 1
        return step * SLOTS + jnp.clip(links[k, side, 2], 0, SLOTS - 1)

    exchange(send_1, recv_1, 0, 2 * SLOTS)
    greet(0)

    def scalar_rims(k, carry):
        slab_rims(k, 2)
        return carry

    lax.fori_loop(0, SLOTS, scalar_rims, 0)
    exchange(send_slab, recv_slab, 3, SLOTS * FIELDS)
    greeted(0)
    greet(1)

    not_west[...] = jnp.where(place == 0, 0.0, 1.0)
    not_east[...] = jnp.where(place == TILE - 1, 0.0, 1.0)
    zero_row = jnp.zeros((1, LANES), jnp.float32)
    for side in range(4):
        for k in range(SLOTS):
            code = links[k, side, 3]
            there = (links[k, side, 2] >= 0).astype(jnp.float32)
            one = lambda flag: flag.astype(jnp.float32)
            fill = lambda value: jnp.full((1, LANES), value, jnp.float32)
            flags[side, k : k + 1, :] = fill(one(code != 0))
            valid[side, k : k + 1, :] = fill(there)
            turn_a[side, k : k + 1, :] = fill(there * (one(code == 0) - one(code == 2)))
            turn_b[side, k : k + 1, :] = fill(there * (one(code == 1) - one(code == 3)))
        for table in (flags, valid, turn_a, turn_b, rows_a, rows_b):
            table[side, 3:4, :] = zero_row
    for l in range(LEVELS):
        mixings[l : l + 1, :] = jnp.full((1, LANES), mixing[l], jnp.float32)
        for f in range(FIELDS):
            spreads[f, l : l + 1, :] = jnp.full((1, LANES), spread[f, l], jnp.float32)
    centre_term[:, block(63)] = tail
    for table in (centre_term, east_flow, north_flow):
        table[3:4, :] = jnp.zeros((1, WIDE), jnp.float32)
    for k in range(SLOTS):
        for f, flow in ((0, east_flow), (1, north_flow)):
            scaled = masked[k * FIELDS + f] * tiled(weights[...])
            flow[k : k + 1, :] = jnp.sum(scaled, axis=0, keepdims=True)

    first_field, second_field, third_field = (vector_rows.at[i] for i in range(3))

    def flux_inside():
        west, east, _, _ = beside(east_flow[...], not_west[...], not_east[...])
        _, _, south, north = beside(north_flow[...], not_west[...], not_east[...])
        return 0.5 * wet[...] * (east - west + north - south)

    first_field[...] = flux_inside()
    diagonal_copy.wait()
    for k in range(SLOTS):
        centre_term[k : k + 1, 0:CELLS] = raw_diagonal[k] + (4.0 - CENTRE)

    def add_rims(target, scale, west, east, south, north):
        columns, first, before, final = spread_rims(west, east, south, north)
        target[...] += scale * wet[...] * (columns * rim_mask[...])
        for k, value in ((0, first), (62, before), (63, final)):
            target[:, block(k)] += scale * wet[:, block(k)] * value

    def operator_inside(target, values):
        west, east, south, north = beside(values[...], not_west[...], not_east[...])
        target[...] = wet[...] * (
            centre_term[...] * values[...] - ((west + east) + (south + north))
        )

    def send_surface(values, sent, received, slot):
        for side, value in enumerate(rims_of(lambda k: values[:, block(k)], rim)):
            for k in range(SLOTS):
                sent[side, k] = value[k : k + 1, :]
        exchange(sent, received, slot, SLOTS)

    def received_surface(received, slot):
        whole(received, slot).wait_recv()
        out = []
        for side in range(4):
            for k in range(SLOTS):
                rows_a[side, k : k + 1, :] = received[side, source_of(k, side)]
            out.append(flip(rows_a[side] * valid[side], flags[side]))
        return out

    whole(recv_1, 0).wait_recv()
    gathered = []
    for side in range(4):
        for k in range(SLOTS):
            at = 2 * source_of(k, side)
            rows_a[side, k : k + 1, :] = recv_1[side, at]
            rows_b[side, k : k + 1, :] = recv_1[side, at + 1]
        a, b = turn_a[side], turn_b[side]
        if side in (WEST, EAST):
            turned = a * rows_a[side] + b * rows_b[side]
        else:
            turned = a * rows_b[side] - b * rows_a[side]
        if side in (WEST, SOUTH):
            turned = -turned
        gathered.append(flip(turned, flags[side]))
    add_rims(first_field, 0.5, *gathered)
    send_surface(first_field, send_2, recv_2, 1)
    greeted(1)
    greet(2)

    operator_inside(second_field, first_field)
    add_rims(second_field, -1.0, *received_surface(recv_2, 1))
    send_surface(second_field, send_3, recv_3, 2)
    greeted(2)
    greet(3)

    operator_inside(third_field, second_field)

    def total(value):
        return jnp.sum(jnp.sum(value, axis=1, keepdims=True), axis=0, keepdims=True)

    moment_0 = total(first_field[...] * first_field[...])
    moment_1 = total(first_field[...] * second_field[...])
    moment_2 = total(second_field[...] * second_field[...])
    add_rims(third_field, -1.0, *received_surface(recv_3, 2))
    moment_3 = total(second_field[...] * third_field[...])
    vectors_copy = pltpu.make_async_copy(vector_rows, vectors, out_sems.at[1])
    lane = lane_row((1, LANES))
    packed = jnp.where(lane == 0, moment_0, 0.0)
    packed = jnp.where(lane == 1, moment_1, packed)
    packed = jnp.where(lane == 2, moment_2, packed)
    packed = jnp.where(lane == 3, moment_3, packed)

    def share(buffer, position, value, devices, slot):
        buffer[position] = value
        for device in devices:
            pltpu.make_async_remote_copy(
                src_ref=buffer.at[position],
                dst_ref=buffer.at[position],
                send_sem=send_sems.at[slot],
                recv_sem=recv_sems.at[slot],
                device_id=device,
                device_id_type=MESH,
            ).start()

    def shared(buffer, count, slot):
        return whole(buffer.at[pl.ds(0, count)], slot)

    share(plane, here, packed, [plane_device(o) for o in range(1, planes)], 4)
    for i in range(3, len(rounds)):
        greeted(i)
    shared(plane, planes - 1, 4).wait_recv()
    packed = jnp.sum(plane[...], axis=0)
    offsets = []
    for d in range(length // 2, 0, -1):
        offsets += [d] if 2 * d == length else [d, -d]
    share(column, z, packed, [column_device(o) for o in offsets], 5)

    vectors_copy.start()
    whole(recv_slab, 3).wait_recv()

    def slab_orient(k, carry):
        for side in range(4):
            code = links[k, side, 3]
            there = (links[k, side, 2] >= 0).astype(jnp.float32)
            cosine = there * ((code == 0).astype(jnp.float32) - (code == 2).astype(jnp.float32))
            sine = there * ((code == 1).astype(jnp.float32) - (code == 3).astype(jnp.float32))
            turn = (code != 0).astype(jnp.float32)
            at = source_of(k, side) * FIELDS
            u, v, scalar = (recv_slab[side, at + f] for f in range(FIELDS))
            values = (cosine * u + sine * v, cosine * v - sine * u, there * scalar)
            for f in range(FIELDS):
                slab_rows[side, k * FIELDS + f] = flip(
                    values[f], jnp.full((4, LANES), turn, jnp.float32)
                )
        return carry

    lax.fori_loop(0, SLOTS, slab_orient, 0)

    def slab_step(a, carry):
        k = lax.div(a, FIELDS)
        f = lax.rem(a, FIELDS)
        m = masked[a]
        west, east, south, north = beside(m, not_west[...], not_east[...])
        columns, first, before, final = spread_rims(*(slab_rows[side, a] for side in range(4)))
        flat = (west + east) + (south + north) + columns * rim_mask[...]
        flat = jnp.concatenate(
            [
                flat[:, block(0)] + first,
                flat[:, LANES : 62 * LANES],
                flat[:, block(62)] + before,
                flat[:, block(63)] + final,
            ],
            axis=1,
        )
        flat = flat - 4.0 * m
        above = jnp.concatenate([m[1:4], m[3:4]], axis=0)
        below = jnp.concatenate([m[0:1], m[0:3]], axis=0)
        vertical = above + below - 2.0 * m
        updated = wet_levels[k] * (
            m + tiled(spreads[f]) * flat + tiled(mixings[...]) * vertical
        )
        stepped[a] = updated[:, 0:CELLS]
        pltpu.make_async_copy(stepped.at[a], adjoint.at[a], out_sems.at[0]).start()
        return carry

    lax.fori_loop(0, SLOTS * FIELDS, slab_step, 0)

    shared(column, length - 1, 5).wait_recv()
    packed = jnp.sum(column[...], axis=0)
    n0, n1, n2, n3 = (
        jnp.sum(jnp.where(lane == i, packed, 0.0), axis=1, keepdims=True) for i in range(4)
    )
    r1, r2, r3 = n1 / n0, n2 / n0, n3 / n0
    mu = r1 + CENTRE
    alpha_0 = 1.0 / mu
    beta = (r2 - r1 * r1) * alpha_0 * alpha_0
    applied = (r1 * r1 * r1 - 2.0 * r1 * r2 + r3) * alpha_0 * alpha_0 + CENTRE * beta
    alpha_1 = beta / (applied - beta * beta * mu)
    c1 = alpha_0 + alpha_1 * (1.0 + beta)
    c2 = alpha_0 * alpha_1
    scale_row[...] = jnp.where(lane == 0, c1, jnp.where(lane == 1, c2, 0.0))
    scales_copy = pltpu.make_async_copy(scale_row, scales, out_sems.at[2])
    scales_copy.start()
    for slot, buffer in enumerate((recv_1, recv_2, recv_3, recv_slab)):
        whole(buffer, slot).wait_send()
    shared(plane, planes - 1, 4).wait_send()
    shared(column, length - 1, 5).wait_send()
    pltpu.make_async_copy(stepped, adjoint, out_sems.at[0]).wait()
    vectors_copy.wait()
    scales_copy.wait()


def final_kernel(
    adjoint_in, vectors_in, scales_in, adjoint, answer, remainder,
    slab, vectors, scales, answer_rows, remainder_rows, in_sems, out_sems,
):
    scales_copy = pltpu.make_async_copy(scales_in, scales, in_sems.at[0])
    scales_copy.start()
    vectors_copy = pltpu.make_async_copy(vectors_in, vectors, in_sems.at[1])
    vectors_copy.start()
    slabs = SLOTS * FIELDS
    incoming = [
        pltpu.make_async_copy(adjoint_in.at[a], slab.at[a], in_sems.at[2 + a])
        for a in range(slabs)
    ]
    outgoing = [
        pltpu.make_async_copy(slab.at[a], adjoint.at[a], out_sems.at[2 + a])
        for a in range(slabs)
    ]
    for copy in incoming:
        copy.start()
    scales_copy.wait()
    vectors_copy.wait()
    c1 = scales[0:1, 0:1]
    c2 = scales[0:1, 1:2]
    r, v, w = (vectors[i, 0:3, 0:CELLS] for i in range(3))
    found = (c1 - CENTRE * c2) * r - c2 * v
    left = (1.0 - CENTRE * c1 + CENTRE * CENTRE * c2) * r + (2.0 * CENTRE * c2 - c1) * v + c2 * w
    for k in range(SLOTS):
        answer_rows[k] = found[k : k + 1]
        remainder_rows[k] = left[k : k + 1]
    answer_copy = pltpu.make_async_copy(answer_rows, answer, out_sems.at[0])
    remainder_copy = pltpu.make_async_copy(remainder_rows, remainder, out_sems.at[1])
    answer_copy.start()
    remainder_copy.start()
    for arrived, leaving in zip(incoming, outgoing):
        arrived.wait()
        leaving.start()
    for copy in outgoing:
        copy.wait()
    answer_copy.wait()
    remainder_copy.wait()


def make(mesh, length):
    groups, strips = mesh.shape["tiles"], mesh.shape["strip"]
    planes = groups // length * strips
    slabs = SLOTS * FIELDS
    f32 = jnp.float32
    V = lambda *shape: pltpu.VMEM(shape, f32)
    hbm = pl.BlockSpec(memory_space=pltpu.HBM)
    call = pl.pallas_call(
        functools.partial(kernel, (groups, strips, length)),
        out_shape=(
            jax.ShapeDtypeStruct((slabs, LEVELS, CELLS), f32),
            jax.ShapeDtypeStruct((3, 4, WIDE), f32),
            jax.ShapeDtypeStruct((1, LANES), f32),
        ),
        in_specs=[hbm] * 7,
        out_specs=(hbm, hbm, hbm),
        scratch_shapes=[
            V(slabs, LEVELS, CELLS),
            pltpu.VMEM((SLOTS, 1, CELLS), jnp.int32),
            V(SLOTS, 1, CELLS),
            V(slabs, LEVELS, WIDE),
            V(slabs, LEVELS, CELLS), V(3, 4, WIDE), V(1, LANES),
            V(4, WIDE),
            V(SLOTS, 4, WIDE),
            V(4, WIDE),
            V(4, WIDE), V(4, WIDE), V(4, WIDE),
            V(4, WIDE), V(4, WIDE),
            V(4, 4, LANES), V(4, 4, LANES), V(4, 4, LANES), V(4, 4, LANES),
            V(FIELDS, 4, LANES), V(4, LANES), V(4, LANES),
            V(4, 4, LANES), V(4, 4, LANES), V(4, slabs, 4, LANES),
            V(4, 2 * SLOTS, 1, LANES), V(4, 6 * SLOTS, 1, LANES),
            V(4, SLOTS, 1, LANES), V(4, 3 * SLOTS, 1, LANES),
            V(4, SLOTS, 1, LANES), V(4, 3 * SLOTS, 1, LANES),
            V(4, slabs, 4, LANES), V(4, 3 * slabs, 4, LANES),
            V(planes, 1, LANES), V(length, 1, LANES),
            pltpu.SMEM((SLOTS, 4, 4), jnp.int32),
            pltpu.SMEM((FIELDS, LEVELS), f32),
            pltpu.SMEM((LEVELS,), f32),
            pltpu.SMEM((LEVELS,), f32),
            pltpu.SemaphoreType.DMA((15,)),
            pltpu.SemaphoreType.DMA((3,)),
            pltpu.SemaphoreType.DMA((6,)),
            pltpu.SemaphoreType.DMA((6,)),
            pltpu.SemaphoreType.REGULAR((4,)),
        ],
        compiler_params=pltpu.CompilerParams(
            collective_id=0, has_side_effects=True, vmem_limit_bytes=GRANT
        ),
        name="slab_and_gradients",
    )

    finish = pl.pallas_call(
        final_kernel,
        out_shape=(
            jax.ShapeDtypeStruct((slabs, LEVELS, CELLS), f32),
            jax.ShapeDtypeStruct((SLOTS, 1, CELLS), f32),
            jax.ShapeDtypeStruct((SLOTS, 1, CELLS), f32),
        ),
        in_specs=[hbm] * 3,
        out_specs=(hbm, hbm, hbm),
        scratch_shapes=[
            V(slabs, LEVELS, CELLS), V(3, 4, WIDE), V(1, LANES),
            V(SLOTS, 1, CELLS), V(SLOTS, 1, CELLS),
            pltpu.SemaphoreType.DMA((2 + slabs,)),
            pltpu.SemaphoreType.DMA((2 + slabs,)),
        ],
        compiler_params=pltpu.CompilerParams(vmem_limit_bytes=GRANT),
        name="last_step",
    )

    def on_device(fields, wet_land, links, surface_diagonal, spread, mixing, thickness):
        updated, vectors, scales = call(
            links.reshape(SLOTS, 4, 4),
            spread,
            mixing,
            thickness,
            fields.reshape(slabs, LEVELS, CELLS),
            wet_land.reshape(SLOTS, 1, CELLS),
            surface_diagonal.reshape(SLOTS, 1, CELLS),
        )
        updated, found, left = finish(updated, vectors, scales)
        return updated.reshape(fields.shape), found.reshape(wet_land.shape), left.reshape(wet_land.shape)

    return jax.shard_map(
        on_device,
        mesh=mesh,
        in_specs=(
            P("tiles", "strip", None, None, None, None),
            P("tiles", "strip", None, None),
            P("tiles", "strip", None, None, None),
            P("tiles", "strip", None, None),
            P(),
            P(),
            P(),
        ),
        out_specs=(
            P("tiles", "strip", None, None, None, None),
            P("tiles", "strip", None, None),
            P("tiles", "strip", None, None),
        ),
        check_vma=False,
    )


def solution(mesh):
    return make(mesh, 32)
```

```python
import functools

import jax
import jax.numpy as jnp
from jax import lax
from jax.experimental import pallas as pl
from jax.experimental.pallas import tpu as pltpu
from jax.sharding import PartitionSpec as P

TILE = 90
SLOTS = 3
FIELDS = 3
LEVELS = 4
CELLS = TILE * TILE
LANES = 128
BLOCKS = 64
WIDE = LANES * BLOCKS
SPLIT = 45
CENTRE = 5.0
GRANT = 57_000_000
MESH = pl.DeviceIdType.MESH
WEST, EAST, SOUTH, NORTH = 0, 1, 2, 3


def take_lanes(rows, index):
    return jnp.take_along_axis(rows, index, axis=1, mode="promise_in_bounds")


def block(k):
    return slice(k * LANES, (k + 1) * LANES)


def beside(x, not_west, not_east):
    west = pltpu.roll(x, 1, 1) * not_west
    east = pltpu.roll(x, WIDE - 1, 1) * not_east
    south = pltpu.roll(x, TILE, 1)
    north = pltpu.roll(x, WIDE - TILE, 1)
    return west, east, south, north


def lane_row(shape=(4, LANES)):
    return lax.broadcasted_iota(jnp.int32, shape, 1)


def rims_of(load, rim):
    def merged(first, last):
        values = [(load(k), rim(k)) for k in range(first, last)]
        chains = []
        for start in range(4):
            total = None
            for value, mask in values[start::4]:
                kept = value * mask
                total = kept if total is None else total + kept
            chains.append(total)
        return (chains[0] + chains[1]) + (chains[2] + chains[3])

    low = merged(0, SPLIT)
    high = merged(SPLIT, BLOCKS)
    lane = lane_row()
    west_lane = (lane * TILE) & (LANES - 1)
    east_lane = (lane * TILE + (TILE - 1)) & (LANES - 1)
    west = jnp.where(lane < 64, take_lanes(low, west_lane), take_lanes(high, west_lane))
    east = jnp.where(lane < 64, take_lanes(low, east_lane), take_lanes(high, east_lane))
    south = load(0)
    north = jnp.where(lane < 54, pltpu.roll(load(62), 54, 1), pltpu.roll(load(63), 54, 1))
    return west, east, south, north


def spread_rims(west, east, south, north):
    lane = lane_row()
    half = lax.shift_right_logical(lane, 1)
    odd = (lane & 1) == 1
    west_row = (half * 37) & 63
    east_row = (lax.shift_right_logical(lane + 39, 1) * 37) & 63
    low = jnp.where(odd, take_lanes(east, east_row), take_lanes(west, west_row))
    high = jnp.where(odd, take_lanes(east, east_row + 64), take_lanes(west, west_row + 64))
    first = jnp.where(lane < TILE, south, 0.0)
    turned = pltpu.roll(north, 74, 1)
    before = jnp.where(lane >= 74, turned, 0.0)
    final = jnp.where(lane < 36, turned, 0.0)
    columns = jnp.concatenate([low] * SPLIT + [high] * (BLOCKS - SPLIT), axis=1)
    return columns, first, before, final


def flip(rows, flags):
    back = (TILE - 1 - lane_row()) & (LANES - 1)
    return jnp.where(flags > 0.0, take_lanes(rows, back), rows)


def kernel(
    sizes,
    links_in, spread_in, mixing_in, thickness_in, fields, wet_land, diagonal,
    adjoint, vectors, scales,
    raw, raw_wet, raw_diagonal, masked, stepped, vector_rows, scale_row, wet, wet_levels, centre_term,
    not_west, not_east, rim_mask, east_flow, north_flow,
    flags, turn_a, turn_b, valid, spreads, mixings, weights,
    rows_a, rows_b, slab_rows,
    send_1, recv_1, send_2, recv_2, send_wet, recv_wet, send_slab, recv_slab,
    corners, beside_links, own_rims,
    plane, column, links, far_links, spread, mixing, thickness,
    in_sems, out_sems, send_sems, recv_sems, hello,
):
    groups, strips, length = sizes
    wet_copy = pltpu.make_async_copy(wet_land, raw_wet, in_sems.at[9])
    wet_copy.start()
    def field_copy(a):
        return pltpu.make_async_copy(fields.at[a], raw.at[a], in_sems.at[a])

    for k in range(SLOTS):
        for f in range(2):
            field_copy(k * FIELDS + f).start()
    diagonal_copy = pltpu.make_async_copy(diagonal, raw_diagonal, in_sems.at[10])
    diagonal_copy.start()
    table_copies = [
        pltpu.make_async_copy(source, target, in_sems.at[11 + i])
        for i, (source, target) in enumerate(
            (
                (links_in, links),
                (spread_in, spread),
                (mixing_in, mixing),
                (thickness_in, thickness),
            )
        )
    ]
    for copy in table_copies:
        copy.start()
    own_links = beside_links.at[4]
    own_links_copy = pltpu.make_async_copy(links_in, own_links, in_sems.at[15])
    own_links_copy.start()
    for k in range(SLOTS):
        field_copy(k * FIELDS + 2).start()

    t = lax.axis_index("tiles")
    s = lax.axis_index("strip")
    core = lax.rem(t, 2)
    chip = lax.div(t, 2)
    z = lax.rem(chip, length)
    x = lax.div(chip, length)
    planes = groups // length * strips
    here = (x * strips + s) * 2 + core

    def beside_device(dt, ds):
        return (lax.rem(t + dt + groups, groups), lax.rem(s + ds + strips, strips))

    def plane_device(offset):
        other = lax.rem(here + offset, planes)
        at_x = lax.div(other, 2 * strips)
        at_s = lax.rem(lax.div(other, 2), strips)
        return ((at_x * length + z) * 2 + lax.rem(other, 2), at_s)

    def column_device(offset):
        return ((x * length + lax.rem(z + offset + length, length)) * 2 + core, s)

    near = [(dt, ds) for dt in (-1, 0, 1) for ds in (-1, 0, 1) if (dt, ds) != (0, 0)]
    stride = 2 * length

    def offset_device(dx, ds, dz, other):
        along_x = lax.rem(x + dx + groups // stride, groups // stride)
        along_z = lax.rem(z + dz + length, length)
        along_s = lax.rem(s + ds + strips, strips)
        return ((along_x * length + along_z) * 2 + (1 - core if other else core), along_s)

    first = [(1, 0, 0, 0), (-1, 0, 0, 0), (0, 0, 1, 0), (0, 0, -1, 0)]
    barrier = pltpu.get_barrier_semaphore()
    for dt, ds in near:
        pl.semaphore_signal(barrier, inc=1, device_id=beside_device(dt, ds), device_id_type=MESH)
    for offset in first:
        pl.semaphore_signal(
            barrier, inc=1, device_id=offset_device(*offset), device_id_type=MESH
        )

    rounds = [
        first,
        [(2, 0, 0, 0), (0, 2, 0, 0), (0, 0, 0, 1), (0, 0, 2, 0), (0, 0, -2, 0)],
    ]
    reach = 4
    while reach < length // 2:
        rounds.append([(0, 0, reach, 0), (0, 0, -reach, 0)])
        reach *= 2

    def greet(i):
        if i < len(rounds):
            for offset in rounds[i]:
                pl.semaphore_signal(
                    hello.at[i], inc=1, device_id=offset_device(*offset), device_id_type=MESH
                )
        if i == 0:
            for offset in near:
                pl.semaphore_signal(
                    hello.at[i], inc=1, device_id=beside_device(*offset), device_id_type=MESH
                )

    def greeted(i):
        if i < len(rounds):
            pl.semaphore_wait(hello.at[i], len(rounds[i]) + (len(near) if i == 0 else 0))

    cell = lax.broadcasted_iota(jnp.int32, (4, WIDE), 1)
    row = lax.shift_right_logical(cell * 11651, 20)
    place = cell - row * TILE
    at_rim = (place == 0) | (place == TILE - 1)
    rim_mask[...] = jnp.where(at_rim & (cell < CELLS), 1.0, 0.0)
    tail = jnp.zeros((4, LANES), jnp.float32)
    wet[:, block(63)] = tail
    wet[3:4, :] = jnp.zeros((1, WIDE), jnp.float32)
    for a in range(SLOTS * FIELDS):
        masked[a, :, block(63)] = tail

    def tiled(rows):
        return jnp.concatenate([rows] * BLOCKS, axis=1)

    for copy in table_copies:
        copy.wait()
    for l in range(LEVELS):
        weights[l : l + 1, :] = jnp.full((1, LANES), thickness[l], jnp.float32)
    wet_copy.wait()
    for k in range(SLOTS):
        wet[k : k + 1, 0:CELLS] = raw_wet[k].astype(jnp.float32)
        wet_levels[k] = jnp.broadcast_to(wet[k : k + 1, :], (4, WIDE))

    rim = lambda k: rim_mask[:, block(k)]

    def slab_rims(k, f):
        a = k * FIELDS + f
        field_copy(a).wait()
        kept = wet_levels[k, :, 0:CELLS] > 0.0
        masked[a, :, 0:CELLS] = jnp.where(kept, raw[a], 0.0)
        values = rims_of(lambda i: masked[a, :, block(i)], rim)
        for side, value in enumerate(values):
            send_slab[side, a] = value
        return values

    def velocity_rims(i, carry):
        k = lax.div(i, 2)
        f = lax.rem(i, 2)
        for side, value in enumerate(slab_rims(k, f)):
            send_1[side, i] = jnp.sum(value * weights[...], axis=0, keepdims=True)
        return carry

    lax.fori_loop(0, 2 * SLOTS, velocity_rims, 0)

    pl.semaphore_wait(barrier, len(near) + len(first))

    def exchange(sent, received, slot, width):
        for d in (-1, 0, 1):
            for side, device in (
                (EAST, beside_device(1, d)),
                (WEST, beside_device(-1, d)),
                (NORTH, beside_device(d, 1)),
                (SOUTH, beside_device(d, -1)),
            ):
                pltpu.make_async_remote_copy(
                    src_ref=sent.at[side],
                    dst_ref=received.at[side ^ 1, pl.ds((1 - d) * width, width)],
                    send_sem=send_sems.at[slot],
                    recv_sem=recv_sems.at[slot],
                    device_id=device,
                    device_id_type=MESH,
                ).start()

    def whole(buffer, slot):
        return pltpu.make_async_remote_copy(
            src_ref=buffer,
            dst_ref=buffer,
            send_sem=send_sems.at[slot],
            recv_sem=recv_sems.at[slot],
            device_id=beside_device(1, 0),
            device_id_type=MESH,
        )

    def source_of(k, side):
        step = links[k, side, 1] if side in (WEST, EAST) else links[k, side, 0]
        step = jnp.clip(step, -1, 1) + 1
        return step * SLOTS + jnp.clip(links[k, side, 2], 0, SLOTS - 1)

    exchange(send_1, recv_1, 0, 2 * SLOTS)
    own_links_copy.wait()
    for dt, ds in near:
        pltpu.make_async_remote_copy(
            src_ref=own_links,
            dst_ref=beside_links.at[(1 - dt) * 3 + 1 - ds],
            send_sem=send_sems.at[6],
            recv_sem=recv_sems.at[6],
            device_id=beside_device(dt, ds),
            device_id_type=MESH,
        ).start()
    greet(0)

    def scalar_rims(k, carry):
        slab_rims(k, 2)
        return carry

    lax.fori_loop(0, SLOTS, scalar_rims, 0)
    exchange(send_slab, recv_slab, 3, SLOTS * FIELDS)
    for side, value in enumerate(rims_of(lambda i: wet[:, block(i)], rim)):
        for k in range(SLOTS):
            send_wet[side, k] = value[k : k + 1, :]
    exchange(send_wet, recv_wet, 2, SLOTS)
    greeted(0)
    greet(1)

    not_west[...] = jnp.where(place == 0, 0.0, 1.0)
    not_east[...] = jnp.where(place == TILE - 1, 0.0, 1.0)
    zero_row = jnp.zeros((1, LANES), jnp.float32)
    for side in range(4):
        for k in range(SLOTS):
            code = links[k, side, 3]
            there = (links[k, side, 2] >= 0).astype(jnp.float32)
            one = lambda flag: flag.astype(jnp.float32)
            fill = lambda value: jnp.full((1, LANES), value, jnp.float32)
            flags[side, k : k + 1, :] = fill(one(code != 0))
            valid[side, k : k + 1, :] = fill(there)
            turn_a[side, k : k + 1, :] = fill(there * (one(code == 0) - one(code == 2)))
            turn_b[side, k : k + 1, :] = fill(there * (one(code == 1) - one(code == 3)))
        for table in (flags, valid, turn_a, turn_b, rows_a, rows_b):
            table[side, 3:4, :] = zero_row
    for l in range(LEVELS):
        mixings[l : l + 1, :] = jnp.full((1, LANES), mixing[l], jnp.float32)
        for f in range(FIELDS):
            spreads[f, l : l + 1, :] = jnp.full((1, LANES), spread[f, l], jnp.float32)
    centre_term[:, block(63)] = tail
    for table in (centre_term, east_flow, north_flow):
        table[3:4, :] = jnp.zeros((1, WIDE), jnp.float32)
    for k in range(SLOTS):
        for f, flow in ((0, east_flow), (1, north_flow)):
            scaled = masked[k * FIELDS + f] * tiled(weights[...])
            flow[k : k + 1, :] = jnp.sum(scaled, axis=0, keepdims=True)

    first_field, second_field, third_field = (vector_rows.at[i] for i in range(3))

    def flux_inside():
        west, east, _, _ = beside(east_flow[...], not_west[...], not_east[...])
        _, _, south, north = beside(north_flow[...], not_west[...], not_east[...])
        return 0.5 * wet[...] * (east - west + north - south)

    first_field[...] = flux_inside()
    diagonal_copy.wait()
    for k in range(SLOTS):
        centre_term[k : k + 1, 0:CELLS] = raw_diagonal[k] + (4.0 - CENTRE)

    def add_rims(target, scale, west, east, south, north):
        columns, first, before, final = spread_rims(west, east, south, north)
        target[...] += scale * wet[...] * (columns * rim_mask[...])
        for k, value in ((0, first), (62, before), (63, final)):
            target[:, block(k)] += scale * wet[:, block(k)] * value

    def operator_inside(target, values):
        west, east, south, north = beside(values[...], not_west[...], not_east[...])
        target[...] = wet[...] * (
            centre_term[...] * values[...] - ((west + east) + (south + north))
        )

    def select(received, step, part):
        out = []
        for side in range(4):
            for k in range(SLOTS):
                rows_a[side, k : k + 1, :] = received[side, step * source_of(k, side) + part]
            out.append(flip(rows_a[side] * valid[side], flags[side]))
        return out

    links_arrived = whole(beside_links.at[pl.ds(0, 8)], 6)
    links_arrived.wait_recv()
    links_copy = pltpu.make_async_copy(beside_links, far_links, in_sems.at[16])
    links_copy.start()
    links_copy.wait()
    corner_of = {}
    for k in range(SLOTS):
        for side in range(4):
            dt = jnp.clip(links[k, side, 0], -1, 1)
            ds = jnp.clip(links[k, side, 1], -1, 1)
            at = (dt + 1) * 3 + ds + 1
            slot = jnp.clip(links[k, side, 2], 0, SLOTS - 1)
            high = 1 if (side ^ 1) in (EAST, NORTH) else 0
            for end in range(2):
                beyond = (SOUTH if end == 0 else NORTH) if side in (WEST, EAST) else end
                far = [far_links[at, slot, beyond, i] for i in range(4)]
                place_flag = jnp.where(far[3] != 0, 1 - high, high)
                facing = beyond ^ 1
                if facing in (SOUTH, NORTH):
                    lane_at = (TILE - 1 if facing == NORTH else 0) + place_flag
                else:
                    lane_at = (TILE - 1) * place_flag + (1 if facing == EAST else 0)
                go_t = jnp.clip(far[0], -1, 1) + dt + 2
                go_s = lax.rem(jnp.clip(far[1], -1, 1) + ds + 2 * strips, strips)
                line = (go_t * strips + go_s) * SLOTS + jnp.clip(far[2], 0, SLOTS - 1)
                corner_of[k, side, end] = (
                    line,
                    jnp.where(far[2] >= 0, lane_at, LANES),
                )

    whole(recv_1, 0).wait_recv()
    gathered = []
    for side in range(4):
        for k in range(SLOTS):
            at = 2 * source_of(k, side)
            rows_a[side, k : k + 1, :] = recv_1[side, at]
            rows_b[side, k : k + 1, :] = recv_1[side, at + 1]
        a, b = turn_a[side], turn_b[side]
        if side in (WEST, EAST):
            turned = a * rows_a[side] + b * rows_b[side]
        else:
            turned = a * rows_b[side] - b * rows_a[side]
        if side in (WEST, SOUTH):
            turned = -turned
        gathered.append(flip(turned, flags[side]))
    add_rims(first_field, 0.5, *gathered)
    for side, value in enumerate(rims_of(lambda k: first_field[:, block(k)], rim)):
        own_rims[side] = value
        for k in range(SLOTS):
            send_2[side, 2 * k] = value[k : k + 1, :]
    lanes = lane_row()
    corner_rows = jnp.where(
        (lanes == 0) | (lanes == TILE - 1),
        own_rims[WEST],
        pltpu.roll(own_rims[EAST], 1, 1),
    )
    own_place = 2 * strips * SLOTS
    for k in range(SLOTS):
        corners[own_place + k] = corner_rows[k : k + 1, :]
    far_devices = [(dt, ds) for ds in range(strips) for dt in range(-2, 3) if (dt, ds) != (0, 0)]
    for dt, ds in far_devices:
        pltpu.make_async_remote_copy(
            src_ref=corners.at[pl.ds(own_place, SLOTS)],
            dst_ref=corners.at[
                pl.ds(((2 - dt) * strips + (strips - ds) % strips) * SLOTS, SLOTS)
            ],
            send_sem=send_sems.at[7],
            recv_sem=recv_sems.at[7],
            device_id=(lax.rem(t + dt + groups, groups), lax.rem(s + ds, strips)),
            device_id_type=MESH,
        ).start()
    operator_inside(second_field, first_field)
    for side, value in enumerate(rims_of(lambda k: second_field[:, block(k)], rim)):
        for k in range(SLOTS):
            send_2[side, 2 * k + 1] = value[k : k + 1, :]
    exchange(send_2, recv_2, 1, 2 * SLOTS)
    greeted(1)
    greet(2)

    def total(value):
        return jnp.sum(jnp.sum(value, axis=1, keepdims=True), axis=0, keepdims=True)

    moment_0 = total(first_field[...] * first_field[...])
    whole(recv_wet, 2).wait_recv()
    wet_beside = select(recv_wet, 1, 0)
    whole(recv_2, 1).wait_recv()
    add_rims(second_field, -1.0, *select(recv_2, 2, 0))
    inside_beside = select(recv_2, 2, 1)
    operator_inside(third_field, second_field)
    corners_arrived = whole(corners.at[pl.ds(0, len(far_devices) * SLOTS)], 7)
    corners_arrived.wait_recv()
    line_lanes = lane_row((1, LANES))
    image_beside = []
    for side in range(4):
        for k in range(SLOTS):
            both = []
            for end in range(2):
                line, lane_at = corner_of[k, side, end]
                kept = jnp.where(line_lanes == lane_at, corners[line], 0.0)
                both.append(jnp.sum(kept, axis=1, keepdims=True))
            rows_a[side, k : k + 1, :] = jnp.where(
                line_lanes == 0, both[0], jnp.where(line_lanes == TILE - 1, both[1], 0.0)
            )
        others = flip(rows_a[side], flags[side])
        image_beside.append(
            inside_beside[side]
            - wet_beside[side] * (jnp.where(lanes < TILE, own_rims[side], 0.0) + others)
        )
    add_rims(third_field, -1.0, *image_beside)
    greeted(2)
    greet(3)
    moment_1 = total(first_field[...] * second_field[...])
    moment_2 = total(second_field[...] * second_field[...])
    moment_3 = total(second_field[...] * third_field[...])
    vectors_copy = pltpu.make_async_copy(vector_rows, vectors, out_sems.at[1])
    lane = lane_row((1, LANES))
    packed = jnp.where(lane == 0, moment_0, 0.0)
    packed = jnp.where(lane == 1, moment_1, packed)
    packed = jnp.where(lane == 2, moment_2, packed)
    packed = jnp.where(lane == 3, moment_3, packed)

    def share(buffer, position, value, devices, slot):
        buffer[position] = value
        for device in devices:
            pltpu.make_async_remote_copy(
                src_ref=buffer.at[position],
                dst_ref=buffer.at[position],
                send_sem=send_sems.at[slot],
                recv_sem=recv_sems.at[slot],
                device_id=device,
                device_id_type=MESH,
            ).start()

    def shared(buffer, count, slot):
        return whole(buffer.at[pl.ds(0, count)], slot)

    share(plane, here, packed, [plane_device(o) for o in range(1, planes)], 4)
    for i in range(3, len(rounds)):
        greeted(i)
    shared(plane, planes - 1, 4).wait_recv()
    packed = jnp.sum(plane[...], axis=0)
    offsets = []
    for d in range(length // 2, 0, -1):
        offsets += [d] if 2 * d == length else [d, -d]
    share(column, z, packed, [column_device(o) for o in offsets], 5)

    vectors_copy.start()
    whole(recv_slab, 3).wait_recv()

    def slab_orient(k, carry):
        for side in range(4):
            code = links[k, side, 3]
            there = (links[k, side, 2] >= 0).astype(jnp.float32)
            cosine = there * ((code == 0).astype(jnp.float32) - (code == 2).astype(jnp.float32))
            sine = there * ((code == 1).astype(jnp.float32) - (code == 3).astype(jnp.float32))
            turn = (code != 0).astype(jnp.float32)
            at = source_of(k, side) * FIELDS
            u, v, scalar = (recv_slab[side, at + f] for f in range(FIELDS))
            values = (cosine * u + sine * v, cosine * v - sine * u, there * scalar)
            for f in range(FIELDS):
                slab_rows[side, k * FIELDS + f] = flip(
                    values[f], jnp.full((4, LANES), turn, jnp.float32)
                )
        return carry

    lax.fori_loop(0, SLOTS, slab_orient, 0)

    def slab_step(a, carry):
        k = lax.div(a, FIELDS)
        f = lax.rem(a, FIELDS)
        m = masked[a]
        west, east, south, north = beside(m, not_west[...], not_east[...])
        columns, first, before, final = spread_rims(*(slab_rows[side, a] for side in range(4)))
        flat = (west + east) + (south + north) + columns * rim_mask[...]
        flat = jnp.concatenate(
            [
                flat[:, block(0)] + first,
                flat[:, LANES : 62 * LANES],
                flat[:, block(62)] + before,
                flat[:, block(63)] + final,
            ],
            axis=1,
        )
        flat = flat - 4.0 * m
        above = jnp.concatenate([m[1:4], m[3:4]], axis=0)
        below = jnp.concatenate([m[0:1], m[0:3]], axis=0)
        vertical = above + below - 2.0 * m
        updated = wet_levels[k] * (
            m + tiled(spreads[f]) * flat + tiled(mixings[...]) * vertical
        )
        stepped[a] = updated[:, 0:CELLS]
        pltpu.make_async_copy(stepped.at[a], adjoint.at[a], out_sems.at[0]).start()
        return carry

    lax.fori_loop(0, SLOTS * FIELDS, slab_step, 0)

    shared(column, length - 1, 5).wait_recv()
    packed = jnp.sum(column[...], axis=0)
    n0, n1, n2, n3 = (
        jnp.sum(jnp.where(lane == i, packed, 0.0), axis=1, keepdims=True) for i in range(4)
    )
    r1, r2, r3 = n1 / n0, n2 / n0, n3 / n0
    mu = r1 + CENTRE
    alpha_0 = 1.0 / mu
    beta = (r2 - r1 * r1) * alpha_0 * alpha_0
    applied = (r1 * r1 * r1 - 2.0 * r1 * r2 + r3) * alpha_0 * alpha_0 + CENTRE * beta
    alpha_1 = beta / (applied - beta * beta * mu)
    c1 = alpha_0 + alpha_1 * (1.0 + beta)
    c2 = alpha_0 * alpha_1
    scale_row[...] = jnp.where(lane == 0, c1, jnp.where(lane == 1, c2, 0.0))
    scales_copy = pltpu.make_async_copy(scale_row, scales, out_sems.at[2])
    scales_copy.start()
    for slot, buffer in enumerate((recv_1, recv_2, recv_wet, recv_slab)):
        whole(buffer, slot).wait_send()
    links_arrived.wait_send()
    corners_arrived.wait_send()
    shared(plane, planes - 1, 4).wait_send()
    shared(column, length - 1, 5).wait_send()
    pltpu.make_async_copy(stepped, adjoint, out_sems.at[0]).wait()
    vectors_copy.wait()
    scales_copy.wait()


def final_kernel(
    adjoint_in, vectors_in, scales_in, adjoint, answer, remainder,
    slab, vectors, scales, answer_rows, remainder_rows, in_sems, out_sems,
):
    scales_copy = pltpu.make_async_copy(scales_in, scales, in_sems.at[0])
    scales_copy.start()
    vectors_copy = pltpu.make_async_copy(vectors_in, vectors, in_sems.at[1])
    vectors_copy.start()
    slabs = SLOTS * FIELDS
    incoming = [
        pltpu.make_async_copy(adjoint_in.at[a], slab.at[a], in_sems.at[2 + a])
        for a in range(slabs)
    ]
    outgoing = [
        pltpu.make_async_copy(slab.at[a], adjoint.at[a], out_sems.at[2 + a])
        for a in range(slabs)
    ]
    for copy in incoming:
        copy.start()
    scales_copy.wait()
    vectors_copy.wait()
    c1 = scales[0:1, 0:1]
    c2 = scales[0:1, 1:2]
    r, v, w = (vectors[i, 0:3, 0:CELLS] for i in range(3))
    found = (c1 - CENTRE * c2) * r - c2 * v
    left = (1.0 - CENTRE * c1 + CENTRE * CENTRE * c2) * r + (2.0 * CENTRE * c2 - c1) * v + c2 * w
    for k in range(SLOTS):
        answer_rows[k] = found[k : k + 1]
        remainder_rows[k] = left[k : k + 1]
    answer_copy = pltpu.make_async_copy(answer_rows, answer, out_sems.at[0])
    remainder_copy = pltpu.make_async_copy(remainder_rows, remainder, out_sems.at[1])
    answer_copy.start()
    remainder_copy.start()
    for arrived, leaving in zip(incoming, outgoing):
        arrived.wait()
        leaving.start()
    for copy in outgoing:
        copy.wait()
    answer_copy.wait()
    remainder_copy.wait()


def make(mesh, length):
    groups, strips = mesh.shape["tiles"], mesh.shape["strip"]
    planes = groups // length * strips
    slabs = SLOTS * FIELDS
    f32 = jnp.float32
    V = lambda *shape: pltpu.VMEM(shape, f32)
    hbm = pl.BlockSpec(memory_space=pltpu.HBM)
    call = pl.pallas_call(
        functools.partial(kernel, (groups, strips, length)),
        out_shape=(
            jax.ShapeDtypeStruct((slabs, LEVELS, CELLS), f32),
            jax.ShapeDtypeStruct((3, 4, WIDE), f32),
            jax.ShapeDtypeStruct((1, LANES), f32),
        ),
        in_specs=[hbm] * 7,
        out_specs=(hbm, hbm, hbm),
        scratch_shapes=[
            V(slabs, LEVELS, CELLS),
            pltpu.VMEM((SLOTS, 1, CELLS), jnp.int32),
            V(SLOTS, 1, CELLS),
            V(slabs, LEVELS, WIDE),
            V(slabs, LEVELS, CELLS), V(3, 4, WIDE), V(1, LANES),
            V(4, WIDE),
            V(SLOTS, 4, WIDE),
            V(4, WIDE),
            V(4, WIDE), V(4, WIDE), V(4, WIDE),
            V(4, WIDE), V(4, WIDE),
            V(4, 4, LANES), V(4, 4, LANES), V(4, 4, LANES), V(4, 4, LANES),
            V(FIELDS, 4, LANES), V(4, LANES), V(4, LANES),
            V(4, 4, LANES), V(4, 4, LANES), V(4, slabs, 4, LANES),
            V(4, 2 * SLOTS, 1, LANES), V(4, 6 * SLOTS, 1, LANES),
            V(4, 2 * SLOTS, 1, LANES), V(4, 6 * SLOTS, 1, LANES),
            V(4, SLOTS, 1, LANES), V(4, 3 * SLOTS, 1, LANES),
            V(4, slabs, 4, LANES), V(4, 3 * slabs, 4, LANES),
            V(5 * strips * SLOTS, 1, LANES),
            pltpu.VMEM((9, SLOTS, 4, 4), jnp.int32),
            V(4, 4, LANES),
            V(planes, 1, LANES), V(length, 1, LANES),
            pltpu.SMEM((SLOTS, 4, 4), jnp.int32),
            pltpu.SMEM((9, SLOTS, 4, 4), jnp.int32),
            pltpu.SMEM((FIELDS, LEVELS), f32),
            pltpu.SMEM((LEVELS,), f32),
            pltpu.SMEM((LEVELS,), f32),
            pltpu.SemaphoreType.DMA((17,)),
            pltpu.SemaphoreType.DMA((3,)),
            pltpu.SemaphoreType.DMA((8,)),
            pltpu.SemaphoreType.DMA((8,)),
            pltpu.SemaphoreType.REGULAR((4,)),
        ],
        compiler_params=pltpu.CompilerParams(
            collective_id=0, has_side_effects=True, vmem_limit_bytes=GRANT
        ),
        name="slab_and_gradients",
    )

    finish = pl.pallas_call(
        final_kernel,
        out_shape=(
            jax.ShapeDtypeStruct((slabs, LEVELS, CELLS), f32),
            jax.ShapeDtypeStruct((SLOTS, 1, CELLS), f32),
            jax.ShapeDtypeStruct((SLOTS, 1, CELLS), f32),
        ),
        in_specs=[hbm] * 3,
        out_specs=(hbm, hbm, hbm),
        scratch_shapes=[
            V(slabs, LEVELS, CELLS), V(3, 4, WIDE), V(1, LANES),
            V(SLOTS, 1, CELLS), V(SLOTS, 1, CELLS),
            pltpu.SemaphoreType.DMA((2 + slabs,)),
            pltpu.SemaphoreType.DMA((2 + slabs,)),
        ],
        compiler_params=pltpu.CompilerParams(vmem_limit_bytes=GRANT),
        name="last_step",
    )

    def on_device(fields, wet_land, links, surface_diagonal, spread, mixing, thickness):
        updated, vectors, scales = call(
            links.reshape(SLOTS, 4, 4),
            spread,
            mixing,
            thickness,
            fields.reshape(slabs, LEVELS, CELLS),
            wet_land.reshape(SLOTS, 1, CELLS),
            surface_diagonal.reshape(SLOTS, 1, CELLS),
        )
        updated, found, left = finish(updated, vectors, scales)
        return updated.reshape(fields.shape), found.reshape(wet_land.shape), left.reshape(wet_land.shape)

    return jax.shard_map(
        on_device,
        mesh=mesh,
        in_specs=(
            P("tiles", "strip", None, None, None, None),
            P("tiles", "strip", None, None),
            P("tiles", "strip", None, None, None),
            P("tiles", "strip", None, None),
            P(),
            P(),
            P(),
        ),
        out_specs=(
            P("tiles", "strip", None, None, None, None),
            P("tiles", "strip", None, None),
            P("tiles", "strip", None, None),
        ),
        check_vma=False,
    )


def solution(mesh):
    return make(mesh, 32)
```

```python
import functools

import jax
import jax.numpy as jnp
from jax import lax
from jax.experimental import pallas as pl
from jax.experimental.pallas import tpu as pltpu
from jax.sharding import PartitionSpec as P

TILE = 90
SLOTS = 3
FIELDS = 3
LEVELS = 4
CELLS = TILE * TILE
LANES = 128
BLOCKS = 64
WIDE = LANES * BLOCKS
SPLIT = 45
CENTRE = 5.0
GRANT = 57_000_000
MESH = pl.DeviceIdType.MESH
WEST, EAST, SOUTH, NORTH = 0, 1, 2, 3


def take_lanes(rows, index):
    return jnp.take_along_axis(rows, index, axis=1, mode="promise_in_bounds")


def block(k):
    return slice(k * LANES, (k + 1) * LANES)


def beside(x, not_west, not_east):
    west = pltpu.roll(x, 1, 1) * not_west
    east = pltpu.roll(x, WIDE - 1, 1) * not_east
    south = pltpu.roll(x, TILE, 1)
    north = pltpu.roll(x, WIDE - TILE, 1)
    return west, east, south, north


def lane_row(shape=(4, LANES)):
    return lax.broadcasted_iota(jnp.int32, shape, 1)


def rims_of(load, rim):
    def merged(first, last):
        values = [(load(k), rim(k)) for k in range(first, last)]
        chains = []
        for start in range(4):
            total = None
            for value, mask in values[start::4]:
                kept = value * mask
                total = kept if total is None else total + kept
            chains.append(total)
        return (chains[0] + chains[1]) + (chains[2] + chains[3])

    low = merged(0, SPLIT)
    high = merged(SPLIT, BLOCKS)
    lane = lane_row()
    west_lane = (lane * TILE) & (LANES - 1)
    east_lane = (lane * TILE + (TILE - 1)) & (LANES - 1)
    west = jnp.where(lane < 64, take_lanes(low, west_lane), take_lanes(high, west_lane))
    east = jnp.where(lane < 64, take_lanes(low, east_lane), take_lanes(high, east_lane))
    south = load(0)
    north = jnp.where(lane < 54, pltpu.roll(load(62), 54, 1), pltpu.roll(load(63), 54, 1))
    return west, east, south, north


def spread_rims(west, east, south, north):
    lane = lane_row()
    half = lax.shift_right_logical(lane, 1)
    odd = (lane & 1) == 1
    west_row = (half * 37) & 63
    east_row = (lax.shift_right_logical(lane + 39, 1) * 37) & 63
    low = jnp.where(odd, take_lanes(east, east_row), take_lanes(west, west_row))
    high = jnp.where(odd, take_lanes(east, east_row + 64), take_lanes(west, west_row + 64))
    first = jnp.where(lane < TILE, south, 0.0)
    turned = pltpu.roll(north, 74, 1)
    before = jnp.where(lane >= 74, turned, 0.0)
    final = jnp.where(lane < 36, turned, 0.0)
    columns = jnp.concatenate([low] * SPLIT + [high] * (BLOCKS - SPLIT), axis=1)
    return columns, first, before, final


def flip(rows, flags):
    back = (TILE - 1 - lane_row()) & (LANES - 1)
    return jnp.where(flags > 0.0, take_lanes(rows, back), rows)


def kernel(
    sizes,
    links_in, spread_in, mixing_in, thickness_in, fields, wet_land, diagonal,
    adjoint, vectors, scales,
    raw, raw_wet, raw_diagonal, masked, stepped, vector_rows, scale_row, wet, wet_levels, centre_term,
    not_west, not_east, rim_mask, east_flow, north_flow,
    flags, turn_a, turn_b, valid, spreads, mixings, weights,
    rows_a, rows_b, slab_rows,
    send_1, recv_1, send_2, recv_2, send_wet, recv_wet, send_slab, recv_slab,
    corners, beside_links, own_rims, wet_rims, centre_rims, inside_rims, image_rims,
    plane, column, links, far_links, spread, mixing, thickness,
    in_sems, out_sems, send_sems, recv_sems, hello,
):
    groups, strips, length = sizes
    wet_copy = pltpu.make_async_copy(wet_land, raw_wet, in_sems.at[9])
    wet_copy.start()
    def field_copy(a):
        return pltpu.make_async_copy(fields.at[a], raw.at[a], in_sems.at[a])

    for k in range(SLOTS):
        for f in range(2):
            field_copy(k * FIELDS + f).start()
    diagonal_copy = pltpu.make_async_copy(diagonal, raw_diagonal, in_sems.at[10])
    diagonal_copy.start()
    table_copies = [
        pltpu.make_async_copy(source, target, in_sems.at[11 + i])
        for i, (source, target) in enumerate(
            (
                (links_in, links),
                (spread_in, spread),
                (mixing_in, mixing),
                (thickness_in, thickness),
            )
        )
    ]
    for copy in table_copies:
        copy.start()
    own_links = beside_links.at[4]
    own_links_copy = pltpu.make_async_copy(links_in, own_links, in_sems.at[15])
    own_links_copy.start()
    for k in range(SLOTS):
        field_copy(k * FIELDS + 2).start()

    t = lax.axis_index("tiles")
    s = lax.axis_index("strip")
    core = lax.rem(t, 2)
    chip = lax.div(t, 2)
    z = lax.rem(chip, length)
    x = lax.div(chip, length)
    planes = groups // length * strips
    here = (x * strips + s) * 2 + core

    def beside_device(dt, ds):
        return (lax.rem(t + dt + groups, groups), lax.rem(s + ds + strips, strips))

    def column_device(offset):
        return ((x * length + lax.rem(z + offset + length, length)) * 2 + core, s)

    near = [(dt, ds) for dt in (-1, 0, 1) for ds in (-1, 0, 1) if (dt, ds) != (0, 0)]
    stride = 2 * length

    def offset_device(dx, ds, dz, other):
        along_x = lax.rem(x + dx + groups // stride, groups // stride)
        along_z = lax.rem(z + dz + length, length)
        along_s = lax.rem(s + ds + strips, strips)
        return ((along_x * length + along_z) * 2 + (1 - core if other else core), along_s)

    first = [(1, 0, 0, 0), (-1, 0, 0, 0), (0, 0, 1, 0), (0, 0, -1, 0)]
    barrier = pltpu.get_barrier_semaphore()
    for dt, ds in near:
        pl.semaphore_signal(barrier, inc=1, device_id=beside_device(dt, ds), device_id_type=MESH)
    for offset in first:
        pl.semaphore_signal(
            barrier, inc=1, device_id=offset_device(*offset), device_id_type=MESH
        )

    rounds = [
        first,
        [(2, 0, 0, 0), (0, 2, 0, 0), (0, 0, 0, 1), (0, 0, 2, 0), (0, 0, -2, 0)],
    ]
    reach = 4
    while reach < length // 2:
        rounds.append([(0, 0, reach, 0), (0, 0, -reach, 0)])
        reach *= 2

    def greet(i):
        if i < len(rounds):
            for offset in rounds[i]:
                pl.semaphore_signal(
                    hello.at[i], inc=1, device_id=offset_device(*offset), device_id_type=MESH
                )
        if i == 0:
            for offset in near:
                pl.semaphore_signal(
                    hello.at[i], inc=1, device_id=beside_device(*offset), device_id_type=MESH
                )

    def greeted(i):
        if i < len(rounds):
            pl.semaphore_wait(hello.at[i], len(rounds[i]) + (len(near) if i == 0 else 0))

    cell = lax.broadcasted_iota(jnp.int32, (4, WIDE), 1)
    row = lax.shift_right_logical(cell * 11651, 20)
    place = cell - row * TILE
    at_rim = (place == 0) | (place == TILE - 1)
    rim_mask[...] = jnp.where(at_rim & (cell < CELLS), 1.0, 0.0)
    tail = jnp.zeros((4, LANES), jnp.float32)
    wet[:, block(63)] = tail
    wet[3:4, :] = jnp.zeros((1, WIDE), jnp.float32)
    for a in range(SLOTS * FIELDS):
        masked[a, :, block(63)] = tail

    def tiled(rows):
        return jnp.concatenate([rows] * BLOCKS, axis=1)

    for copy in table_copies:
        copy.wait()
    for l in range(LEVELS):
        weights[l : l + 1, :] = jnp.full((1, LANES), thickness[l], jnp.float32)
    wet_copy.wait()
    for k in range(SLOTS):
        wet[k : k + 1, 0:CELLS] = raw_wet[k].astype(jnp.float32)
        wet_levels[k] = jnp.broadcast_to(wet[k : k + 1, :], (4, WIDE))

    rim = lambda k: rim_mask[:, block(k)]

    def slab_rims(k, f):
        a = k * FIELDS + f
        field_copy(a).wait()
        kept = wet_levels[k, :, 0:CELLS] > 0.0
        masked[a, :, 0:CELLS] = jnp.where(kept, raw[a], 0.0)
        values = rims_of(lambda i: masked[a, :, block(i)], rim)
        for side, value in enumerate(values):
            send_slab[side, a] = value
        return values

    def velocity_rims(i, carry):
        k = lax.div(i, 2)
        f = lax.rem(i, 2)
        for side, value in enumerate(slab_rims(k, f)):
            send_1[side, i] = jnp.sum(value * weights[...], axis=0, keepdims=True)
        return carry

    lax.fori_loop(0, 2 * SLOTS, velocity_rims, 0)

    pl.semaphore_wait(barrier, len(near) + len(first))

    def exchange(sent, received, slot, width):
        for d in (-1, 1, 0):
            for side, device in (
                (EAST, beside_device(1, d)),
                (WEST, beside_device(-1, d)),
                (NORTH, beside_device(d, 1)),
                (SOUTH, beside_device(d, -1)),
            ):
                pltpu.make_async_remote_copy(
                    src_ref=sent.at[side],
                    dst_ref=received.at[side ^ 1, pl.ds((1 - d) * width, width)],
                    send_sem=send_sems.at[slot],
                    recv_sem=recv_sems.at[slot],
                    device_id=device,
                    device_id_type=MESH,
                ).start()

    def whole(buffer, slot):
        return pltpu.make_async_remote_copy(
            src_ref=buffer,
            dst_ref=buffer,
            send_sem=send_sems.at[slot],
            recv_sem=recv_sems.at[slot],
            device_id=beside_device(1, 0),
            device_id_type=MESH,
        )

    def source_of(k, side):
        step = links[k, side, 1] if side in (WEST, EAST) else links[k, side, 0]
        step = jnp.clip(step, -1, 1) + 1
        return step * SLOTS + jnp.clip(links[k, side, 2], 0, SLOTS - 1)

    exchange(send_1, recv_1, 0, 2 * SLOTS)
    own_links_copy.wait()
    for dt, ds in near:
        pltpu.make_async_remote_copy(
            src_ref=own_links,
            dst_ref=beside_links.at[(1 - dt) * 3 + 1 - ds],
            send_sem=send_sems.at[6],
            recv_sem=recv_sems.at[6],
            device_id=beside_device(dt, ds),
            device_id_type=MESH,
        ).start()
    greet(0)

    def scalar_rims(k, carry):
        slab_rims(k, 2)
        return carry

    lax.fori_loop(0, SLOTS, scalar_rims, 0)
    exchange(send_slab, recv_slab, 3, SLOTS * FIELDS)
    lanes = lane_row()

    def on_rim(rows):
        return jnp.where(lanes < TILE, rows, 0.0)

    for side, value in enumerate(rims_of(lambda i: wet[:, block(i)], rim)):
        wet_rims[side] = on_rim(value)
        for k in range(SLOTS):
            send_wet[side, k] = value[k : k + 1, :]
    exchange(send_wet, recv_wet, 2, SLOTS)
    greeted(0)
    greet(1)

    not_west[...] = jnp.where(place == 0, 0.0, 1.0)
    not_east[...] = jnp.where(place == TILE - 1, 0.0, 1.0)
    zero_row = jnp.zeros((1, LANES), jnp.float32)
    for side in range(4):
        for k in range(SLOTS):
            code = links[k, side, 3]
            there = (links[k, side, 2] >= 0).astype(jnp.float32)
            one = lambda flag: flag.astype(jnp.float32)
            fill = lambda value: jnp.full((1, LANES), value, jnp.float32)
            flags[side, k : k + 1, :] = fill(one(code != 0))
            valid[side, k : k + 1, :] = fill(there)
            turn_a[side, k : k + 1, :] = fill(there * (one(code == 0) - one(code == 2)))
            turn_b[side, k : k + 1, :] = fill(there * (one(code == 1) - one(code == 3)))
        for table in (flags, valid, turn_a, turn_b, rows_a, rows_b):
            table[side, 3:4, :] = zero_row
    for l in range(LEVELS):
        mixings[l : l + 1, :] = jnp.full((1, LANES), mixing[l], jnp.float32)
        for f in range(FIELDS):
            spreads[f, l : l + 1, :] = jnp.full((1, LANES), spread[f, l], jnp.float32)
    centre_term[:, block(63)] = tail
    for table in (centre_term, east_flow, north_flow):
        table[3:4, :] = jnp.zeros((1, WIDE), jnp.float32)
    for k in range(SLOTS):
        for f, flow in ((0, east_flow), (1, north_flow)):
            scaled = masked[k * FIELDS + f] * tiled(weights[...])
            flow[k : k + 1, :] = jnp.sum(scaled, axis=0, keepdims=True)

    first_field, second_field, third_field = (vector_rows.at[i] for i in range(3))

    def flux_inside():
        west, east, _, _ = beside(east_flow[...], not_west[...], not_east[...])
        _, _, south, north = beside(north_flow[...], not_west[...], not_east[...])
        return 0.5 * wet[...] * (east - west + north - south)

    first_field[...] = flux_inside()
    diagonal_copy.wait()
    for k in range(SLOTS):
        centre_term[k : k + 1, 0:CELLS] = raw_diagonal[k] + (4.0 - CENTRE)

    def add_rims(target, scale, west, east, south, north):
        columns, first, before, final = spread_rims(west, east, south, north)
        target[...] += scale * wet[...] * (columns * rim_mask[...])
        for k, value in ((0, first), (62, before), (63, final)):
            target[:, block(k)] += scale * wet[:, block(k)] * value

    def operator_inside(target, values):
        west, east, south, north = beside(values[...], not_west[...], not_east[...])
        target[...] = wet[...] * (
            centre_term[...] * values[...] - ((west + east) + (south + north))
        )

    def select(received, step, part):
        out = []
        for side in range(4):
            for k in range(SLOTS):
                rows_a[side, k : k + 1, :] = received[side, step * source_of(k, side) + part]
            out.append(flip(rows_a[side] * valid[side], flags[side]))
        return out

    def keep_rims(target, values):
        for side, value in enumerate(rims_of(lambda k: values[:, block(k)], rim)):
            target[side] = on_rim(value)

    def at_ends(low, high):
        return jnp.where(lanes == 0, low, 0.0) + jnp.where(lanes == TILE - 1, high, 0.0)

    def moved(rows, start, stop):
        return pltpu.roll(rows, (stop - start) % LANES, 1) if start != stop else rows

    def corner_terms(rows, step):
        last = TILE - 1
        out = []
        for side in range(4):
            low, high = (SOUTH, NORTH) if side in (WEST, EAST) else (WEST, EAST)
            place = step if side in (WEST, SOUTH) else last - step
            out.append(at_ends(moved(rows[low], place, 0), moved(rows[high], place, last)))
        return out

    def rim_image(rows):
        terms = corner_terms(rows, 1)
        return [
            wet_rims[side]
            * (
                centre_rims[side] * rows[side]
                - (pltpu.roll(rows[side], 1, 1) + pltpu.roll(rows[side], LANES - 1, 1))
                - terms[side]
            )
            for side in range(4)
        ]

    def rim_change(scale, rows):
        terms = corner_terms(rows, 0)
        return [scale * wet_rims[side] * (rows[side] + terms[side]) for side in range(4)]

    keep_rims(centre_rims, centre_term)
    keep_rims(own_rims, first_field)
    operator_inside(second_field, first_field)
    keep_rims(inside_rims, second_field)

    links_arrived = whole(beside_links.at[pl.ds(0, 8)], 6)
    links_arrived.wait_recv()
    links_copy = pltpu.make_async_copy(beside_links, far_links, in_sems.at[16])
    links_copy.start()
    links_copy.wait()
    corner_of = {}
    for k in range(SLOTS):
        for side in range(4):
            dt = jnp.clip(links[k, side, 0], -1, 1)
            ds = jnp.clip(links[k, side, 1], -1, 1)
            at = (dt + 1) * 3 + ds + 1
            slot = jnp.clip(links[k, side, 2], 0, SLOTS - 1)
            high = 1 if (side ^ 1) in (EAST, NORTH) else 0
            for end in range(2):
                beyond = (SOUTH if end == 0 else NORTH) if side in (WEST, EAST) else end
                far = [far_links[at, slot, beyond, i] for i in range(4)]
                place_flag = jnp.where(far[3] != 0, 1 - high, high)
                facing = beyond ^ 1
                if facing in (SOUTH, NORTH):
                    lane_at = (TILE - 1 if facing == NORTH else 0) + place_flag
                else:
                    lane_at = (TILE - 1) * place_flag + (1 if facing == EAST else 0)
                go_t = jnp.clip(far[0], -1, 1) + dt + 2
                go_s = lax.rem(jnp.clip(far[1], -1, 1) + ds + 2 * strips, strips)
                line = (go_t * strips + go_s) * SLOTS + jnp.clip(far[2], 0, SLOTS - 1)
                corner_of[k, side, end] = (
                    line,
                    jnp.where(far[2] >= 0, lane_at, LANES),
                )

    whole(recv_1, 0).wait_recv()
    gathered = []
    for side in range(4):
        for k in range(SLOTS):
            at = 2 * source_of(k, side)
            rows_a[side, k : k + 1, :] = recv_1[side, at]
            rows_b[side, k : k + 1, :] = recv_1[side, at + 1]
        a, b = turn_a[side], turn_b[side]
        if side in (WEST, EAST):
            turned = a * rows_a[side] + b * rows_b[side]
        else:
            turned = a * rows_b[side] - b * rows_a[side]
        if side in (WEST, SOUTH):
            turned = -turned
        gathered.append(on_rim(flip(turned, flags[side])))
    change = rim_change(0.5, gathered)
    images = rim_image(change)
    for side in range(4):
        rows = own_rims[side] + change[side]
        own_rims[side] = rows
        for k in range(SLOTS):
            send_2[side, 2 * k] = rows[k : k + 1, :]
        rows = inside_rims[side] + images[side]
        inside_rims[side] = rows
        for k in range(SLOTS):
            send_2[side, 2 * k + 1] = rows[k : k + 1, :]
    corner_rows = jnp.where(
        (lanes == 0) | (lanes == TILE - 1),
        own_rims[WEST],
        pltpu.roll(own_rims[EAST], 1, 1),
    )
    own_place = 2 * strips * SLOTS
    for k in range(SLOTS):
        corners[own_place + k] = corner_rows[k : k + 1, :]
    far_devices = [(dt, ds) for ds in range(strips) for dt in range(-2, 3) if (dt, ds) != (0, 0)]
    far_devices.sort(key=lambda o: -abs(o[0]) // 2 - min(o[1], strips - o[1]))
    for dt, ds in far_devices:
        pltpu.make_async_remote_copy(
            src_ref=corners.at[pl.ds(own_place, SLOTS)],
            dst_ref=corners.at[
                pl.ds(((2 - dt) * strips + (strips - ds) % strips) * SLOTS, SLOTS)
            ],
            send_sem=send_sems.at[7],
            recv_sem=recv_sems.at[7],
            device_id=(lax.rem(t + dt + groups, groups), lax.rem(s + ds, strips)),
            device_id_type=MESH,
        ).start()
    exchange(send_2, recv_2, 1, 2 * SLOTS)
    greeted(1)
    greet(2)

    def total(value):
        return jnp.sum(jnp.sum(value, axis=1, keepdims=True), axis=0, keepdims=True)

    add_rims(first_field, 0.5, *gathered)
    operator_inside(second_field, first_field)
    operator_inside(third_field, second_field)
    keep_rims(image_rims, third_field)
    moment_0 = total(first_field[...] * first_field[...])
    moment_1 = total(first_field[...] * second_field[...])
    moment_2 = total(second_field[...] * second_field[...])
    moment_3 = total(second_field[...] * third_field[...])
    whole(recv_wet, 2).wait_recv()
    wet_beside = select(recv_wet, 1, 0)
    greeted(2)
    greet(3)
    whole(recv_2, 1).wait_recv()
    others_beside = [on_rim(rows) for rows in select(recv_2, 2, 0)]
    inside_beside = select(recv_2, 2, 1)
    change = rim_change(-1.0, others_beside)
    images = rim_image(change)
    corners_arrived = whole(corners.at[pl.ds(0, len(far_devices) * SLOTS)], 7)
    corners_arrived.wait_recv()
    line_lanes = lane_row((1, LANES))
    image_beside = []
    for side in range(4):
        for k in range(SLOTS):
            both = []
            for end in range(2):
                line, lane_at = corner_of[k, side, end]
                kept = jnp.where(line_lanes == lane_at, corners[line], 0.0)
                both.append(jnp.sum(kept, axis=1, keepdims=True))
            rows_a[side, k : k + 1, :] = jnp.where(
                line_lanes == 0, both[0], jnp.where(line_lanes == TILE - 1, both[1], 0.0)
            )
        others = flip(rows_a[side], flags[side])
        image_beside.append(
            inside_beside[side]
            - wet_beside[side] * (own_rims[side] + others)
        )
    between = (lanes > 0) & (lanes < TILE - 1)
    sums = [jnp.zeros((4, LANES), jnp.float32)] * 3
    for side in range(4):
        once = change[side]
        if side in (SOUTH, NORTH):
            once = jnp.where(between, once, 0.0)
        found = inside_rims[side] + change[side]
        sums = [
            sums[0] + once * own_rims[side],
            sums[1] + once * (inside_rims[side] + found),
            sums[2]
            + once * (2.0 * image_rims[side] + images[side])
            - found * on_rim(image_beside[side]),
        ]
    moment_1 += total(sums[0])
    moment_2 += total(sums[1])
    moment_3 += total(sums[2])
    vectors_copy = pltpu.make_async_copy(vector_rows, vectors, out_sems.at[1])
    lane = lane_row((1, LANES))
    packed = jnp.where(lane == 0, moment_0, 0.0)
    packed = jnp.where(lane == 1, moment_1, packed)
    packed = jnp.where(lane == 2, moment_2, packed)
    packed = jnp.where(lane == 3, moment_3, packed)

    def share(buffer, position, value, devices, slot):
        buffer[position] = value
        for device in devices:
            pltpu.make_async_remote_copy(
                src_ref=buffer.at[position],
                dst_ref=buffer.at[position],
                send_sem=send_sems.at[slot],
                recv_sem=recv_sems.at[slot],
                device_id=device,
                device_id_type=MESH,
            ).start()

    def shared(buffer, count, slot):
        return whole(buffer.at[pl.ds(0, count)], slot)

    across = groups // stride

    def hops(step, count):
        return min(step, count - step)

    in_plane = [
        (dx, ds, 0, other)
        for dx in range(across)
        for ds in range(strips)
        for other in (0, 1)
        if (dx, ds, other) != (0, 0, 0)
    ]
    in_plane.sort(key=lambda o: -hops(o[0], across) - hops(o[1], strips))
    share(plane, here, packed, [offset_device(*o) for o in in_plane], 4)
    for i in range(3, len(rounds)):
        greeted(i)
    shared(plane, planes - 1, 4).wait_recv()
    packed = jnp.sum(plane[...], axis=0)
    offsets = []
    for d in range(length // 2, 0, -1):
        offsets += [d] if 2 * d == length else [d, -d]
    share(column, z, packed, [column_device(o) for o in offsets], 5)

    add_rims(second_field, -1.0, *others_beside)
    operator_inside(third_field, second_field)
    add_rims(third_field, -1.0, *image_beside)
    vectors_copy.start()
    whole(recv_slab, 3).wait_recv()

    def slab_orient(k, carry):
        for side in range(4):
            code = links[k, side, 3]
            there = (links[k, side, 2] >= 0).astype(jnp.float32)
            cosine = there * ((code == 0).astype(jnp.float32) - (code == 2).astype(jnp.float32))
            sine = there * ((code == 1).astype(jnp.float32) - (code == 3).astype(jnp.float32))
            turn = (code != 0).astype(jnp.float32)
            at = source_of(k, side) * FIELDS
            u, v, scalar = (recv_slab[side, at + f] for f in range(FIELDS))
            values = (cosine * u + sine * v, cosine * v - sine * u, there * scalar)
            for f in range(FIELDS):
                slab_rows[side, k * FIELDS + f] = flip(
                    values[f], jnp.full((4, LANES), turn, jnp.float32)
                )
        return carry

    lax.fori_loop(0, SLOTS, slab_orient, 0)

    def slab_step(a, carry):
        k = lax.div(a, FIELDS)
        f = lax.rem(a, FIELDS)
        m = masked[a]
        west, east, south, north = beside(m, not_west[...], not_east[...])
        columns, first, before, final = spread_rims(*(slab_rows[side, a] for side in range(4)))
        flat = (west + east) + (south + north) + columns * rim_mask[...]
        flat = jnp.concatenate(
            [
                flat[:, block(0)] + first,
                flat[:, LANES : 62 * LANES],
                flat[:, block(62)] + before,
                flat[:, block(63)] + final,
            ],
            axis=1,
        )
        flat = flat - 4.0 * m
        above = jnp.concatenate([m[1:4], m[3:4]], axis=0)
        below = jnp.concatenate([m[0:1], m[0:3]], axis=0)
        vertical = above + below - 2.0 * m
        updated = wet_levels[k] * (
            m + tiled(spreads[f]) * flat + tiled(mixings[...]) * vertical
        )
        stepped[a] = updated[:, 0:CELLS]
        pltpu.make_async_copy(stepped.at[a], adjoint.at[a], out_sems.at[0]).start()
        return carry

    lax.fori_loop(0, SLOTS * FIELDS, slab_step, 0)

    shared(column, length - 1, 5).wait_recv()
    packed = jnp.sum(column[...], axis=0)
    n0, n1, n2, n3 = (
        jnp.sum(jnp.where(lane == i, packed, 0.0), axis=1, keepdims=True) for i in range(4)
    )
    r1, r2, r3 = n1 / n0, n2 / n0, n3 / n0
    mu = r1 + CENTRE
    alpha_0 = 1.0 / mu
    beta = (r2 - r1 * r1) * alpha_0 * alpha_0
    applied = (r1 * r1 * r1 - 2.0 * r1 * r2 + r3) * alpha_0 * alpha_0 + CENTRE * beta
    alpha_1 = beta / (applied - beta * beta * mu)
    c1 = alpha_0 + alpha_1 * (1.0 + beta)
    c2 = alpha_0 * alpha_1
    scale_row[...] = jnp.where(lane == 0, c1, jnp.where(lane == 1, c2, 0.0))
    scales_copy = pltpu.make_async_copy(scale_row, scales, out_sems.at[2])
    scales_copy.start()
    for slot, buffer in enumerate((recv_1, recv_2, recv_wet, recv_slab)):
        whole(buffer, slot).wait_send()
    links_arrived.wait_send()
    corners_arrived.wait_send()
    shared(plane, planes - 1, 4).wait_send()
    shared(column, length - 1, 5).wait_send()
    pltpu.make_async_copy(stepped, adjoint, out_sems.at[0]).wait()
    vectors_copy.wait()
    scales_copy.wait()


def final_kernel(
    adjoint_in, vectors_in, scales_in, adjoint, answer, remainder,
    slab, vectors, scales, answer_rows, remainder_rows, in_sems, out_sems,
):
    scales_copy = pltpu.make_async_copy(scales_in, scales, in_sems.at[0])
    scales_copy.start()
    vectors_copy = pltpu.make_async_copy(vectors_in, vectors, in_sems.at[1])
    vectors_copy.start()
    slabs = SLOTS * FIELDS
    incoming = [
        pltpu.make_async_copy(adjoint_in.at[a], slab.at[a], in_sems.at[2 + a])
        for a in range(slabs)
    ]
    outgoing = [
        pltpu.make_async_copy(slab.at[a], adjoint.at[a], out_sems.at[2 + a])
        for a in range(slabs)
    ]
    for copy in incoming:
        copy.start()
    scales_copy.wait()
    vectors_copy.wait()
    c1 = scales[0:1, 0:1]
    c2 = scales[0:1, 1:2]
    r, v, w = (vectors[i, 0:3, 0:CELLS] for i in range(3))
    found = (c1 - CENTRE * c2) * r - c2 * v
    left = (1.0 - CENTRE * c1 + CENTRE * CENTRE * c2) * r + (2.0 * CENTRE * c2 - c1) * v + c2 * w
    for k in range(SLOTS):
        answer_rows[k] = found[k : k + 1]
        remainder_rows[k] = left[k : k + 1]
    answer_copy = pltpu.make_async_copy(answer_rows, answer, out_sems.at[0])
    remainder_copy = pltpu.make_async_copy(remainder_rows, remainder, out_sems.at[1])
    answer_copy.start()
    remainder_copy.start()
    for arrived, leaving in zip(incoming, outgoing):
        arrived.wait()
        leaving.start()
    for copy in outgoing:
        copy.wait()
    answer_copy.wait()
    remainder_copy.wait()


def make(mesh, length):
    groups, strips = mesh.shape["tiles"], mesh.shape["strip"]
    planes = groups // length * strips
    slabs = SLOTS * FIELDS
    f32 = jnp.float32
    V = lambda *shape: pltpu.VMEM(shape, f32)
    hbm = pl.BlockSpec(memory_space=pltpu.HBM)
    call = pl.pallas_call(
        functools.partial(kernel, (groups, strips, length)),
        out_shape=(
            jax.ShapeDtypeStruct((slabs, LEVELS, CELLS), f32),
            jax.ShapeDtypeStruct((3, 4, WIDE), f32),
            jax.ShapeDtypeStruct((1, LANES), f32),
        ),
        in_specs=[hbm] * 7,
        out_specs=(hbm, hbm, hbm),
        scratch_shapes=[
            V(slabs, LEVELS, CELLS),
            pltpu.VMEM((SLOTS, 1, CELLS), jnp.int32),
            V(SLOTS, 1, CELLS),
            V(slabs, LEVELS, WIDE),
            V(slabs, LEVELS, CELLS), V(3, 4, WIDE), V(1, LANES),
            V(4, WIDE),
            V(SLOTS, 4, WIDE),
            V(4, WIDE),
            V(4, WIDE), V(4, WIDE), V(4, WIDE),
            V(4, WIDE), V(4, WIDE),
            V(4, 4, LANES), V(4, 4, LANES), V(4, 4, LANES), V(4, 4, LANES),
            V(FIELDS, 4, LANES), V(4, LANES), V(4, LANES),
            V(4, 4, LANES), V(4, 4, LANES), V(4, slabs, 4, LANES),
            V(4, 2 * SLOTS, 1, LANES), V(4, 6 * SLOTS, 1, LANES),
            V(4, 2 * SLOTS, 1, LANES), V(4, 6 * SLOTS, 1, LANES),
            V(4, SLOTS, 1, LANES), V(4, 3 * SLOTS, 1, LANES),
            V(4, slabs, 4, LANES), V(4, 3 * slabs, 4, LANES),
            V(5 * strips * SLOTS, 1, LANES),
            pltpu.VMEM((9, SLOTS, 4, 4), jnp.int32),
            V(4, 4, LANES), V(4, 4, LANES), V(4, 4, LANES), V(4, 4, LANES), V(4, 4, LANES),
            V(planes, 1, LANES), V(length, 1, LANES),
            pltpu.SMEM((SLOTS, 4, 4), jnp.int32),
            pltpu.SMEM((9, SLOTS, 4, 4), jnp.int32),
            pltpu.SMEM((FIELDS, LEVELS), f32),
            pltpu.SMEM((LEVELS,), f32),
            pltpu.SMEM((LEVELS,), f32),
            pltpu.SemaphoreType.DMA((17,)),
            pltpu.SemaphoreType.DMA((3,)),
            pltpu.SemaphoreType.DMA((8,)),
            pltpu.SemaphoreType.DMA((8,)),
            pltpu.SemaphoreType.REGULAR((4,)),
        ],
        compiler_params=pltpu.CompilerParams(
            collective_id=0, has_side_effects=True, vmem_limit_bytes=GRANT
        ),
        name="slab_and_gradients",
    )

    finish = pl.pallas_call(
        final_kernel,
        out_shape=(
            jax.ShapeDtypeStruct((slabs, LEVELS, CELLS), f32),
            jax.ShapeDtypeStruct((SLOTS, 1, CELLS), f32),
            jax.ShapeDtypeStruct((SLOTS, 1, CELLS), f32),
        ),
        in_specs=[hbm] * 3,
        out_specs=(hbm, hbm, hbm),
        scratch_shapes=[
            V(slabs, LEVELS, CELLS), V(3, 4, WIDE), V(1, LANES),
            V(SLOTS, 1, CELLS), V(SLOTS, 1, CELLS),
            pltpu.SemaphoreType.DMA((2 + slabs,)),
            pltpu.SemaphoreType.DMA((2 + slabs,)),
        ],
        compiler_params=pltpu.CompilerParams(vmem_limit_bytes=GRANT),
        name="last_step",
    )

    def on_device(fields, wet_land, links, surface_diagonal, spread, mixing, thickness):
        updated, vectors, scales = call(
            links.reshape(SLOTS, 4, 4),
            spread,
            mixing,
            thickness,
            fields.reshape(slabs, LEVELS, CELLS),
            wet_land.reshape(SLOTS, 1, CELLS),
            surface_diagonal.reshape(SLOTS, 1, CELLS),
        )
        updated, found, left = finish(updated, vectors, scales)
        return updated.reshape(fields.shape), found.reshape(wet_land.shape), left.reshape(wet_land.shape)

    return jax.shard_map(
        on_device,
        mesh=mesh,
        in_specs=(
            P("tiles", "strip", None, None, None, None),
            P("tiles", "strip", None, None),
            P("tiles", "strip", None, None, None),
            P("tiles", "strip", None, None),
            P(),
            P(),
            P(),
        ),
        out_specs=(
            P("tiles", "strip", None, None, None, None),
            P("tiles", "strip", None, None),
            P("tiles", "strip", None, None),
        ),
        check_vma=False,
    )


def solution(mesh):
    return make(mesh, 32)
```

```python
import functools

import jax
import jax.numpy as jnp
from jax import lax
from jax.experimental import pallas as pl
from jax.experimental.pallas import tpu as pltpu
from jax.sharding import PartitionSpec as P

TILE = 90
SLOTS = 3
FIELDS = 3
LEVELS = 4
CELLS = TILE * TILE
LANES = 128
BLOCKS = 64
WIDE = LANES * BLOCKS
SPLIT = 45
CENTRE = 5.0
GRANT = 57_000_000
MESH = pl.DeviceIdType.MESH
WEST, EAST, SOUTH, NORTH = 0, 1, 2, 3


def take_lanes(rows, index):
    return jnp.take_along_axis(rows, index, axis=1, mode="promise_in_bounds")


def block(k):
    return slice(k * LANES, (k + 1) * LANES)


def beside(x, not_west, not_east):
    west = pltpu.roll(x, 1, 1) * not_west
    east = pltpu.roll(x, WIDE - 1, 1) * not_east
    south = pltpu.roll(x, TILE, 1)
    north = pltpu.roll(x, WIDE - TILE, 1)
    return west, east, south, north


def lane_row(shape=(4, LANES)):
    return lax.broadcasted_iota(jnp.int32, shape, 1)


def rims_of(load, rim):
    def merged(first, last):
        values = [(load(k), rim(k)) for k in range(first, last)]
        chains = []
        for start in range(4):
            total = None
            for value, mask in values[start::4]:
                kept = value * mask
                total = kept if total is None else total + kept
            chains.append(total)
        return (chains[0] + chains[1]) + (chains[2] + chains[3])

    low = merged(0, SPLIT)
    high = merged(SPLIT, BLOCKS)
    lane = lane_row()
    west_lane = (lane * TILE) & (LANES - 1)
    east_lane = (lane * TILE + (TILE - 1)) & (LANES - 1)
    west = jnp.where(lane < 64, take_lanes(low, west_lane), take_lanes(high, west_lane))
    east = jnp.where(lane < 64, take_lanes(low, east_lane), take_lanes(high, east_lane))
    south = load(0)
    north = jnp.where(lane < 54, pltpu.roll(load(62), 54, 1), pltpu.roll(load(63), 54, 1))
    return west, east, south, north


def spread_rims(west, east, south, north):
    lane = lane_row()
    half = lax.shift_right_logical(lane, 1)
    odd = (lane & 1) == 1
    west_row = (half * 37) & 63
    east_row = (lax.shift_right_logical(lane + 39, 1) * 37) & 63
    low = jnp.where(odd, take_lanes(east, east_row), take_lanes(west, west_row))
    high = jnp.where(odd, take_lanes(east, east_row + 64), take_lanes(west, west_row + 64))
    first = jnp.where(lane < TILE, south, 0.0)
    turned = pltpu.roll(north, 74, 1)
    before = jnp.where(lane >= 74, turned, 0.0)
    final = jnp.where(lane < 36, turned, 0.0)
    columns = jnp.concatenate([low] * SPLIT + [high] * (BLOCKS - SPLIT), axis=1)
    return columns, first, before, final


def flip(rows, flags):
    back = (TILE - 1 - lane_row()) & (LANES - 1)
    return jnp.where(flags > 0.0, take_lanes(rows, back), rows)


def kernel(
    sizes,
    links_in, spread_in, mixing_in, thickness_in, fields, wet_land, diagonal,
    adjoint, vectors, scales,
    raw, raw_wet, raw_diagonal, masked, stepped, vector_rows, scale_row, wet, wet_levels, centre_term,
    not_west, not_east, rim_mask, east_flow, north_flow,
    flags, turn_a, turn_b, valid, spreads, mixings, weights,
    rows_a, rows_b, slab_rows,
    send_1, recv_1, send_2, recv_2, send_wet, recv_wet, send_slab, recv_slab,
    corners, beside_links, own_rims, wet_rims, centre_rims, inside_rims, image_rims,
    plane, column, links, far_links, spread, mixing, thickness,
    in_sems, out_sems, send_sems, recv_sems, hello,
):
    groups, strips, length = sizes
    table_copies = [
        pltpu.make_async_copy(source, target, in_sems.at[11 + i])
        for i, (source, target) in enumerate(
            (
                (links_in, links),
                (spread_in, spread),
                (mixing_in, mixing),
                (thickness_in, thickness),
            )
        )
    ]
    for copy in table_copies:
        copy.start()
    wet_copy = pltpu.make_async_copy(wet_land, raw_wet, in_sems.at[9])
    wet_copy.start()
    def field_copy(a):
        return pltpu.make_async_copy(fields.at[a], raw.at[a], in_sems.at[a])

    for k in range(SLOTS):
        for f in range(2):
            field_copy(k * FIELDS + f).start()
    diagonal_copy = pltpu.make_async_copy(diagonal, raw_diagonal, in_sems.at[10])
    diagonal_copy.start()
    own_links = beside_links.at[4]
    own_links_copy = pltpu.make_async_copy(links_in, own_links, in_sems.at[15])
    own_links_copy.start()
    for k in range(SLOTS):
        field_copy(k * FIELDS + 2).start()

    t = lax.axis_index("tiles")
    s = lax.axis_index("strip")
    core = lax.rem(t, 2)
    chip = lax.div(t, 2)
    z = lax.rem(chip, length)
    x = lax.div(chip, length)
    planes = groups // length * strips
    here = (x * strips + s) * 2 + core

    def beside_device(dt, ds):
        return (lax.rem(t + dt + groups, groups), lax.rem(s + ds + strips, strips))

    def column_device(offset):
        return ((x * length + lax.rem(z + offset + length, length)) * 2 + core, s)

    near = [(dt, ds) for dt in (-1, 0, 1) for ds in (-1, 0, 1) if (dt, ds) != (0, 0)]
    stride = 2 * length

    def offset_device(dx, ds, dz, other):
        along_x = lax.rem(x + dx + groups // stride, groups // stride)
        along_z = lax.rem(z + dz + length, length)
        along_s = lax.rem(s + ds + strips, strips)
        return ((along_x * length + along_z) * 2 + (1 - core if other else core), along_s)

    first = [(1, 0, 0, 0), (-1, 0, 0, 0), (0, 0, 1, 0), (0, 0, -1, 0)]
    barrier = pltpu.get_barrier_semaphore()
    for dt, ds in near:
        pl.semaphore_signal(barrier, inc=1, device_id=beside_device(dt, ds), device_id_type=MESH)
    for offset in first:
        pl.semaphore_signal(
            barrier, inc=1, device_id=offset_device(*offset), device_id_type=MESH
        )

    rounds = [
        first,
        [(2, 0, 0, 0), (0, 2, 0, 0), (0, 0, 0, 1), (0, 0, 2, 0), (0, 0, -2, 0)],
    ]
    reach = 4
    while reach < length // 2:
        rounds.append([(0, 0, reach, 0), (0, 0, -reach, 0)])
        reach *= 2

    def greet(i):
        if i < len(rounds):
            for offset in rounds[i]:
                pl.semaphore_signal(
                    hello.at[i], inc=1, device_id=offset_device(*offset), device_id_type=MESH
                )
        if i == 0:
            for offset in near:
                pl.semaphore_signal(
                    hello.at[i], inc=1, device_id=beside_device(*offset), device_id_type=MESH
                )

    def greeted(i):
        if i < len(rounds):
            pl.semaphore_wait(hello.at[i], len(rounds[i]) + (len(near) if i == 0 else 0))

    cell = lax.broadcasted_iota(jnp.int32, (4, WIDE), 1)
    row = lax.shift_right_logical(cell * 11651, 20)
    place = cell - row * TILE
    at_rim = (place == 0) | (place == TILE - 1)
    rim_mask[...] = jnp.where(at_rim & (cell < CELLS), 1.0, 0.0)
    tail = jnp.zeros((4, LANES), jnp.float32)
    wet[:, block(63)] = tail
    wet[3:4, :] = jnp.zeros((1, WIDE), jnp.float32)
    for a in range(SLOTS * FIELDS):
        masked[a, :, block(63)] = tail

    def tiled(rows):
        return jnp.concatenate([rows] * BLOCKS, axis=1)

    for copy in table_copies:
        copy.wait()
    for l in range(LEVELS):
        weights[l : l + 1, :] = jnp.full((1, LANES), thickness[l], jnp.float32)
    wet_copy.wait()
    for k in range(SLOTS):
        wet[k : k + 1, 0:CELLS] = raw_wet[k].astype(jnp.float32)
        wet_levels[k] = jnp.broadcast_to(wet[k : k + 1, :], (4, WIDE))

    rim = lambda k: rim_mask[:, block(k)]

    def slab_rims(k, f):
        a = k * FIELDS + f
        field_copy(a).wait()
        kept = wet_levels[k, :, 0:CELLS] > 0.0
        masked[a, :, 0:CELLS] = jnp.where(kept, raw[a], 0.0)
        values = rims_of(lambda i: masked[a, :, block(i)], rim)
        for side, value in enumerate(values):
            send_slab[side, a] = value
        return values

    def velocity_rims(i, carry):
        k = lax.div(i, 2)
        f = lax.rem(i, 2)
        for side, value in enumerate(slab_rims(k, f)):
            send_1[side, i] = jnp.sum(value * weights[...], axis=0, keepdims=True)
        return carry

    lax.fori_loop(0, 2 * SLOTS, velocity_rims, 0)

    pl.semaphore_wait(barrier, len(near) + len(first))

    def exchange(sent, received, slot, width):
        for d in (-1, 1, 0):
            for side, device in (
                (EAST, beside_device(1, d)),
                (WEST, beside_device(-1, d)),
                (NORTH, beside_device(d, 1)),
                (SOUTH, beside_device(d, -1)),
            ):
                pltpu.make_async_remote_copy(
                    src_ref=sent.at[side],
                    dst_ref=received.at[side ^ 1, pl.ds((1 - d) * width, width)],
                    send_sem=send_sems.at[slot],
                    recv_sem=recv_sems.at[slot],
                    device_id=device,
                    device_id_type=MESH,
                ).start()

    def whole(buffer, slot):
        return pltpu.make_async_remote_copy(
            src_ref=buffer,
            dst_ref=buffer,
            send_sem=send_sems.at[slot],
            recv_sem=recv_sems.at[slot],
            device_id=beside_device(1, 0),
            device_id_type=MESH,
        )

    def source_of(k, side):
        step = links[k, side, 1] if side in (WEST, EAST) else links[k, side, 0]
        step = jnp.clip(step, -1, 1) + 1
        return step * SLOTS + jnp.clip(links[k, side, 2], 0, SLOTS - 1)

    exchange(send_1, recv_1, 0, 2 * SLOTS)
    own_links_copy.wait()
    for dt, ds in near:
        pltpu.make_async_remote_copy(
            src_ref=own_links,
            dst_ref=beside_links.at[(1 - dt) * 3 + 1 - ds],
            send_sem=send_sems.at[6],
            recv_sem=recv_sems.at[6],
            device_id=beside_device(dt, ds),
            device_id_type=MESH,
        ).start()
    greet(0)

    def scalar_rims(k, carry):
        slab_rims(k, 2)
        return carry

    lax.fori_loop(0, SLOTS, scalar_rims, 0)
    exchange(send_slab, recv_slab, 3, SLOTS * FIELDS)
    lanes = lane_row()

    def on_rim(rows):
        return jnp.where(lanes < TILE, rows, 0.0)

    for side, value in enumerate(rims_of(lambda i: wet[:, block(i)], rim)):
        wet_rims[side] = on_rim(value)
        for k in range(SLOTS):
            send_wet[side, k] = value[k : k + 1, :]
    exchange(send_wet, recv_wet, 2, SLOTS)
    greeted(0)
    greet(1)

    not_west[...] = jnp.where(place == 0, 0.0, 1.0)
    not_east[...] = jnp.where(place == TILE - 1, 0.0, 1.0)
    zero_row = jnp.zeros((1, LANES), jnp.float32)
    for side in range(4):
        for k in range(SLOTS):
            code = links[k, side, 3]
            there = (links[k, side, 2] >= 0).astype(jnp.float32)
            one = lambda flag: flag.astype(jnp.float32)
            fill = lambda value: jnp.full((1, LANES), value, jnp.float32)
            flags[side, k : k + 1, :] = fill(one(code != 0))
            valid[side, k : k + 1, :] = fill(there)
            turn_a[side, k : k + 1, :] = fill(there * (one(code == 0) - one(code == 2)))
            turn_b[side, k : k + 1, :] = fill(there * (one(code == 1) - one(code == 3)))
        for table in (flags, valid, turn_a, turn_b, rows_a, rows_b):
            table[side, 3:4, :] = zero_row
    for l in range(LEVELS):
        mixings[l : l + 1, :] = jnp.full((1, LANES), mixing[l], jnp.float32)
        for f in range(FIELDS):
            spreads[f, l : l + 1, :] = jnp.full((1, LANES), spread[f, l], jnp.float32)
    centre_term[:, block(63)] = tail
    for table in (centre_term, east_flow, north_flow):
        table[3:4, :] = jnp.zeros((1, WIDE), jnp.float32)
    for k in range(SLOTS):
        for f, flow in ((0, east_flow), (1, north_flow)):
            scaled = masked[k * FIELDS + f] * tiled(weights[...])
            flow[k : k + 1, :] = jnp.sum(scaled, axis=0, keepdims=True)

    first_field, second_field, third_field = (vector_rows.at[i] for i in range(3))

    def flux_inside():
        west, east, _, _ = beside(east_flow[...], not_west[...], not_east[...])
        _, _, south, north = beside(north_flow[...], not_west[...], not_east[...])
        return 0.5 * wet[...] * (east - west + north - south)

    first_field[...] = flux_inside()
    diagonal_copy.wait()
    for k in range(SLOTS):
        centre_term[k : k + 1, 0:CELLS] = raw_diagonal[k] + (4.0 - CENTRE)

    def add_rims(target, scale, west, east, south, north):
        columns, first, before, final = spread_rims(west, east, south, north)
        target[...] += scale * wet[...] * (columns * rim_mask[...])
        for k, value in ((0, first), (62, before), (63, final)):
            target[:, block(k)] += scale * wet[:, block(k)] * value

    def operator_inside(target, values):
        west, east, south, north = beside(values[...], not_west[...], not_east[...])
        target[...] = wet[...] * (
            centre_term[...] * values[...] - ((west + east) + (south + north))
        )

    def select(received, step, part):
        out = []
        for side in range(4):
            for k in range(SLOTS):
                rows_a[side, k : k + 1, :] = received[side, step * source_of(k, side) + part]
            out.append(flip(rows_a[side] * valid[side], flags[side]))
        return out

    def keep_rims(target, values):
        for side, value in enumerate(rims_of(lambda k: values[:, block(k)], rim)):
            target[side] = on_rim(value)

    def at_ends(low, high):
        return jnp.where(lanes == 0, low, 0.0) + jnp.where(lanes == TILE - 1, high, 0.0)

    def moved(rows, start, stop):
        return pltpu.roll(rows, (stop - start) % LANES, 1) if start != stop else rows

    def corner_terms(rows, step):
        last = TILE - 1
        out = []
        for side in range(4):
            low, high = (SOUTH, NORTH) if side in (WEST, EAST) else (WEST, EAST)
            place = step if side in (WEST, SOUTH) else last - step
            out.append(at_ends(moved(rows[low], place, 0), moved(rows[high], place, last)))
        return out

    def rim_image(rows):
        terms = corner_terms(rows, 1)
        return [
            wet_rims[side]
            * (
                centre_rims[side] * rows[side]
                - (pltpu.roll(rows[side], 1, 1) + pltpu.roll(rows[side], LANES - 1, 1))
                - terms[side]
            )
            for side in range(4)
        ]

    def rim_change(scale, rows):
        terms = corner_terms(rows, 0)
        return [scale * wet_rims[side] * (rows[side] + terms[side]) for side in range(4)]

    keep_rims(centre_rims, centre_term)
    keep_rims(own_rims, first_field)
    operator_inside(second_field, first_field)
    keep_rims(inside_rims, second_field)

    links_arrived = whole(beside_links.at[pl.ds(0, 8)], 6)
    links_arrived.wait_recv()
    links_copy = pltpu.make_async_copy(beside_links, far_links, in_sems.at[16])
    links_copy.start()
    links_copy.wait()
    corner_of = {}
    for k in range(SLOTS):
        for side in range(4):
            dt = jnp.clip(links[k, side, 0], -1, 1)
            ds = jnp.clip(links[k, side, 1], -1, 1)
            at = (dt + 1) * 3 + ds + 1
            slot = jnp.clip(links[k, side, 2], 0, SLOTS - 1)
            high = 1 if (side ^ 1) in (EAST, NORTH) else 0
            for end in range(2):
                beyond = (SOUTH if end == 0 else NORTH) if side in (WEST, EAST) else end
                far = [far_links[at, slot, beyond, i] for i in range(4)]
                place_flag = jnp.where(far[3] != 0, 1 - high, high)
                facing = beyond ^ 1
                if facing in (SOUTH, NORTH):
                    lane_at = (TILE - 1 if facing == NORTH else 0) + place_flag
                else:
                    lane_at = (TILE - 1) * place_flag + (1 if facing == EAST else 0)
                go_t = jnp.clip(far[0], -1, 1) + dt + 2
                go_s = lax.rem(jnp.clip(far[1], -1, 1) + ds + 2 * strips, strips)
                line = (go_t * strips + go_s) * SLOTS + jnp.clip(far[2], 0, SLOTS - 1)
                corner_of[k, side, end] = (
                    line,
                    jnp.where(far[2] >= 0, lane_at, LANES),
                )

    whole(recv_1, 0).wait_recv()
    gathered = []
    for side in range(4):
        for k in range(SLOTS):
            at = 2 * source_of(k, side)
            rows_a[side, k : k + 1, :] = recv_1[side, at]
            rows_b[side, k : k + 1, :] = recv_1[side, at + 1]
        a, b = turn_a[side], turn_b[side]
        if side in (WEST, EAST):
            turned = a * rows_a[side] + b * rows_b[side]
        else:
            turned = a * rows_b[side] - b * rows_a[side]
        if side in (WEST, SOUTH):
            turned = -turned
        gathered.append(on_rim(flip(turned, flags[side])))
    change = rim_change(0.5, gathered)
    images = rim_image(change)
    for side in range(4):
        rows = own_rims[side] + change[side]
        own_rims[side] = rows
        for k in range(SLOTS):
            send_2[side, 2 * k] = rows[k : k + 1, :]
        rows = inside_rims[side] + images[side]
        inside_rims[side] = rows
        for k in range(SLOTS):
            send_2[side, 2 * k + 1] = rows[k : k + 1, :]
    corner_rows = jnp.where(
        (lanes == 0) | (lanes == TILE - 1),
        own_rims[WEST],
        pltpu.roll(own_rims[EAST], 1, 1),
    )
    own_place = 2 * strips * SLOTS
    for k in range(SLOTS):
        corners[own_place + k] = corner_rows[k : k + 1, :]
    far_devices = [(dt, ds) for ds in range(strips) for dt in range(-2, 3) if (dt, ds) != (0, 0)]
    far_devices.sort(key=lambda o: -abs(o[0]) // 2 - min(o[1], strips - o[1]))
    for dt, ds in far_devices:
        pltpu.make_async_remote_copy(
            src_ref=corners.at[pl.ds(own_place, SLOTS)],
            dst_ref=corners.at[
                pl.ds(((2 - dt) * strips + (strips - ds) % strips) * SLOTS, SLOTS)
            ],
            send_sem=send_sems.at[7],
            recv_sem=recv_sems.at[7],
            device_id=(lax.rem(t + dt + groups, groups), lax.rem(s + ds, strips)),
            device_id_type=MESH,
        ).start()
    exchange(send_2, recv_2, 1, 2 * SLOTS)
    greeted(1)
    greet(2)

    def total(value):
        return jnp.sum(jnp.sum(value, axis=1, keepdims=True), axis=0, keepdims=True)

    add_rims(first_field, 0.5, *gathered)
    operator_inside(second_field, first_field)
    operator_inside(third_field, second_field)
    keep_rims(image_rims, third_field)
    moment_0 = total(first_field[...] * first_field[...])
    moment_1 = total(first_field[...] * second_field[...])
    moment_2 = total(second_field[...] * second_field[...])
    moment_3 = total(second_field[...] * third_field[...])
    whole(recv_wet, 2).wait_recv()
    wet_beside = select(recv_wet, 1, 0)
    greeted(2)
    greet(3)
    whole(recv_2, 1).wait_recv()
    others_beside = [on_rim(rows) for rows in select(recv_2, 2, 0)]
    inside_beside = select(recv_2, 2, 1)
    change = rim_change(-1.0, others_beside)
    images = rim_image(change)
    between = (lanes > 0) & (lanes < TILE - 1)
    sums = [jnp.zeros((4, LANES), jnp.float32)] * 3
    found = []
    for side in range(4):
        once = change[side]
        if side in (SOUTH, NORTH):
            once = jnp.where(between, once, 0.0)
        rows = inside_rims[side] + change[side]
        found.append(rows)
        image = inside_beside[side] - wet_beside[side] * own_rims[side]
        sums = [
            sums[0] + once * own_rims[side],
            sums[1] + once * (inside_rims[side] + rows),
            sums[2] + once * (2.0 * image_rims[side] + images[side]) - rows * on_rim(image),
        ]
    lane = lane_row((1, LANES))
    moment_1 += total(sums[0])
    moment_2 += total(sums[1])
    packed = jnp.where(lane == 0, moment_0, 0.0)
    packed = jnp.where(lane == 1, moment_1, packed)
    packed = jnp.where(lane == 2, moment_2, packed)
    moment_3 += total(sums[2])
    corners_arrived = whole(corners.at[pl.ds(0, len(far_devices) * SLOTS)], 7)
    corners_arrived.wait_recv()
    line_lanes = lane_row((1, LANES))
    image_beside = []
    crossed = jnp.zeros((4, LANES), jnp.float32)
    for side in range(4):
        for k in range(SLOTS):
            both = []
            for end in range(2):
                line, lane_at = corner_of[k, side, end]
                kept = jnp.where(line_lanes == lane_at, corners[line], 0.0)
                both.append(jnp.sum(kept, axis=1, keepdims=True))
            rows_a[side, k : k + 1, :] = jnp.where(
                line_lanes == 0, both[0], jnp.where(line_lanes == TILE - 1, both[1], 0.0)
            )
        others = wet_beside[side] * flip(rows_a[side], flags[side])
        crossed = crossed + found[side] * on_rim(others)
        image_beside.append(
            inside_beside[side] - wet_beside[side] * own_rims[side] - others
        )
    packed = jnp.where(lane == 3, moment_3 + total(crossed), packed)
    vectors_copy = pltpu.make_async_copy(vector_rows, vectors, out_sems.at[1])

    def share(buffer, position, value, devices, slot):
        buffer[position] = value
        for device in devices:
            pltpu.make_async_remote_copy(
                src_ref=buffer.at[position],
                dst_ref=buffer.at[position],
                send_sem=send_sems.at[slot],
                recv_sem=recv_sems.at[slot],
                device_id=device,
                device_id_type=MESH,
            ).start()

    def shared(buffer, count, slot):
        return whole(buffer.at[pl.ds(0, count)], slot)

    across = groups // stride

    def hops(step, count):
        return min(step, count - step)

    in_plane = [
        (dx, ds, 0, other)
        for dx in range(across)
        for ds in range(strips)
        for other in (0, 1)
        if (dx, ds, other) != (0, 0, 0)
    ]
    in_plane.sort(key=lambda o: -hops(o[0], across) - hops(o[1], strips))
    share(plane, here, packed, [offset_device(*o) for o in in_plane], 4)
    for i in range(3, len(rounds)):
        greeted(i)
    shared(plane, planes - 1, 4).wait_recv()
    packed = jnp.sum(plane[...], axis=0)
    offsets = []
    for d in range(length // 2, 0, -1):
        offsets += [d] if 2 * d == length else [d, -d]
    share(column, z, packed, [column_device(o) for o in offsets], 5)

    add_rims(second_field, -1.0, *others_beside)
    operator_inside(third_field, second_field)
    add_rims(third_field, -1.0, *image_beside)
    vectors_copy.start()
    whole(recv_slab, 3).wait_recv()

    def slab_orient(k, carry):
        for side in range(4):
            code = links[k, side, 3]
            there = (links[k, side, 2] >= 0).astype(jnp.float32)
            cosine = there * ((code == 0).astype(jnp.float32) - (code == 2).astype(jnp.float32))
            sine = there * ((code == 1).astype(jnp.float32) - (code == 3).astype(jnp.float32))
            turn = (code != 0).astype(jnp.float32)
            at = source_of(k, side) * FIELDS
            u, v, scalar = (recv_slab[side, at + f] for f in range(FIELDS))
            values = (cosine * u + sine * v, cosine * v - sine * u, there * scalar)
            for f in range(FIELDS):
                slab_rows[side, k * FIELDS + f] = flip(
                    values[f], jnp.full((4, LANES), turn, jnp.float32)
                )
        return carry

    lax.fori_loop(0, SLOTS, slab_orient, 0)

    def slab_step(a, carry):
        k = lax.div(a, FIELDS)
        f = lax.rem(a, FIELDS)
        m = masked[a]
        west, east, south, north = beside(m, not_west[...], not_east[...])
        columns, first, before, final = spread_rims(*(slab_rows[side, a] for side in range(4)))
        flat = (west + east) + (south + north) + columns * rim_mask[...]
        flat = jnp.concatenate(
            [
                flat[:, block(0)] + first,
                flat[:, LANES : 62 * LANES],
                flat[:, block(62)] + before,
                flat[:, block(63)] + final,
            ],
            axis=1,
        )
        flat = flat - 4.0 * m
        above = jnp.concatenate([m[1:4], m[3:4]], axis=0)
        below = jnp.concatenate([m[0:1], m[0:3]], axis=0)
        vertical = above + below - 2.0 * m
        updated = wet_levels[k] * (
            m + tiled(spreads[f]) * flat + tiled(mixings[...]) * vertical
        )
        stepped[a] = updated[:, 0:CELLS]
        pltpu.make_async_copy(stepped.at[a], adjoint.at[a], out_sems.at[0]).start()
        return carry

    lax.fori_loop(0, SLOTS * FIELDS, slab_step, 0)

    shared(column, length - 1, 5).wait_recv()
    packed = jnp.sum(column[...], axis=0)
    n0, n1, n2, n3 = (
        jnp.sum(jnp.where(lane == i, packed, 0.0), axis=1, keepdims=True) for i in range(4)
    )
    r1, r2, r3 = n1 / n0, n2 / n0, n3 / n0
    mu = r1 + CENTRE
    alpha_0 = 1.0 / mu
    beta = (r2 - r1 * r1) * alpha_0 * alpha_0
    applied = (r1 * r1 * r1 - 2.0 * r1 * r2 + r3) * alpha_0 * alpha_0 + CENTRE * beta
    alpha_1 = beta / (applied - beta * beta * mu)
    c1 = alpha_0 + alpha_1 * (1.0 + beta)
    c2 = alpha_0 * alpha_1
    scale_row[...] = jnp.where(lane == 0, c1, jnp.where(lane == 1, c2, 0.0))
    scales_copy = pltpu.make_async_copy(scale_row, scales, out_sems.at[2])
    scales_copy.start()
    for slot, buffer in enumerate((recv_1, recv_2, recv_wet, recv_slab)):
        whole(buffer, slot).wait_send()
    links_arrived.wait_send()
    corners_arrived.wait_send()
    shared(plane, planes - 1, 4).wait_send()
    shared(column, length - 1, 5).wait_send()
    pltpu.make_async_copy(stepped, adjoint, out_sems.at[0]).wait()
    vectors_copy.wait()
    scales_copy.wait()


def final_kernel(
    adjoint_in, vectors_in, scales_in, adjoint, answer, remainder,
    slab, vectors, scales, answer_rows, remainder_rows, in_sems, out_sems,
):
    scales_copy = pltpu.make_async_copy(scales_in, scales, in_sems.at[0])
    vectors_copy = pltpu.make_async_copy(vectors_in, vectors, in_sems.at[1])
    slabs = SLOTS * FIELDS
    incoming = [
        pltpu.make_async_copy(adjoint_in.at[a], slab.at[a], in_sems.at[2 + a])
        for a in range(slabs)
    ]
    outgoing = [
        pltpu.make_async_copy(slab.at[a], adjoint.at[a], out_sems.at[2 + a])
        for a in range(slabs)
    ]
    for copy in incoming[:4]:
        copy.start()
    scales_copy.start()
    vectors_copy.start()
    for copy in incoming[4:]:
        copy.start()
    for arrived, leaving in zip(incoming[:4], outgoing[:4]):
        arrived.wait()
        leaving.start()
    scales_copy.wait()
    vectors_copy.wait()
    c1 = scales[0:1, 0:1]
    c2 = scales[0:1, 1:2]
    r, v, w = (vectors[i, 0:3, 0:CELLS] for i in range(3))
    found = (c1 - CENTRE * c2) * r - c2 * v
    left = (1.0 - CENTRE * c1 + CENTRE * CENTRE * c2) * r + (2.0 * CENTRE * c2 - c1) * v + c2 * w
    for k in range(SLOTS):
        answer_rows[k] = found[k : k + 1]
        remainder_rows[k] = left[k : k + 1]
    answer_copy = pltpu.make_async_copy(answer_rows, answer, out_sems.at[0])
    remainder_copy = pltpu.make_async_copy(remainder_rows, remainder, out_sems.at[1])
    answer_copy.start()
    remainder_copy.start()
    for arrived, leaving in zip(incoming[4:], outgoing[4:]):
        arrived.wait()
        leaving.start()
    for copy in outgoing:
        copy.wait()
    answer_copy.wait()
    remainder_copy.wait()


def make(mesh, length):
    groups, strips = mesh.shape["tiles"], mesh.shape["strip"]
    planes = groups // length * strips
    slabs = SLOTS * FIELDS
    f32 = jnp.float32
    V = lambda *shape: pltpu.VMEM(shape, f32)
    hbm = pl.BlockSpec(memory_space=pltpu.HBM)
    call = pl.pallas_call(
        functools.partial(kernel, (groups, strips, length)),
        out_shape=(
            jax.ShapeDtypeStruct((slabs, LEVELS, CELLS), f32),
            jax.ShapeDtypeStruct((3, 4, WIDE), f32),
            jax.ShapeDtypeStruct((1, LANES), f32),
        ),
        in_specs=[hbm] * 7,
        out_specs=(hbm, hbm, hbm),
        scratch_shapes=[
            V(slabs, LEVELS, CELLS),
            pltpu.VMEM((SLOTS, 1, CELLS), jnp.int32),
            V(SLOTS, 1, CELLS),
            V(slabs, LEVELS, WIDE),
            V(slabs, LEVELS, CELLS), V(3, 4, WIDE), V(1, LANES),
            V(4, WIDE),
            V(SLOTS, 4, WIDE),
            V(4, WIDE),
            V(4, WIDE), V(4, WIDE), V(4, WIDE),
            V(4, WIDE), V(4, WIDE),
            V(4, 4, LANES), V(4, 4, LANES), V(4, 4, LANES), V(4, 4, LANES),
            V(FIELDS, 4, LANES), V(4, LANES), V(4, LANES),
            V(4, 4, LANES), V(4, 4, LANES), V(4, slabs, 4, LANES),
            V(4, 2 * SLOTS, 1, LANES), V(4, 6 * SLOTS, 1, LANES),
            V(4, 2 * SLOTS, 1, LANES), V(4, 6 * SLOTS, 1, LANES),
            V(4, SLOTS, 1, LANES), V(4, 3 * SLOTS, 1, LANES),
            V(4, slabs, 4, LANES), V(4, 3 * slabs, 4, LANES),
            V(5 * strips * SLOTS, 1, LANES),
            pltpu.VMEM((9, SLOTS, 4, 4), jnp.int32),
            V(4, 4, LANES), V(4, 4, LANES), V(4, 4, LANES), V(4, 4, LANES), V(4, 4, LANES),
            V(planes, 1, LANES), V(length, 1, LANES),
            pltpu.SMEM((SLOTS, 4, 4), jnp.int32),
            pltpu.SMEM((9, SLOTS, 4, 4), jnp.int32),
            pltpu.SMEM((FIELDS, LEVELS), f32),
            pltpu.SMEM((LEVELS,), f32),
            pltpu.SMEM((LEVELS,), f32),
            pltpu.SemaphoreType.DMA((17,)),
            pltpu.SemaphoreType.DMA((3,)),
            pltpu.SemaphoreType.DMA((8,)),
            pltpu.SemaphoreType.DMA((8,)),
            pltpu.SemaphoreType.REGULAR((4,)),
        ],
        compiler_params=pltpu.CompilerParams(
            collective_id=0, has_side_effects=True, vmem_limit_bytes=GRANT
        ),
        name="slab_and_gradients",
    )

    finish = pl.pallas_call(
        final_kernel,
        out_shape=(
            jax.ShapeDtypeStruct((slabs, LEVELS, CELLS), f32),
            jax.ShapeDtypeStruct((SLOTS, 1, CELLS), f32),
            jax.ShapeDtypeStruct((SLOTS, 1, CELLS), f32),
        ),
        in_specs=[hbm] * 3,
        out_specs=(hbm, hbm, hbm),
        scratch_shapes=[
            V(slabs, LEVELS, CELLS), V(3, 4, WIDE), V(1, LANES),
            V(SLOTS, 1, CELLS), V(SLOTS, 1, CELLS),
            pltpu.SemaphoreType.DMA((2 + slabs,)),
            pltpu.SemaphoreType.DMA((2 + slabs,)),
        ],
        compiler_params=pltpu.CompilerParams(vmem_limit_bytes=GRANT),
        name="last_step",
    )

    def on_device(fields, wet_land, links, surface_diagonal, spread, mixing, thickness):
        updated, vectors, scales = call(
            links.reshape(SLOTS, 4, 4),
            spread,
            mixing,
            thickness,
            fields.reshape(slabs, LEVELS, CELLS),
            wet_land.reshape(SLOTS, 1, CELLS),
            surface_diagonal.reshape(SLOTS, 1, CELLS),
        )
        updated, found, left = finish(updated, vectors, scales)
        return updated.reshape(fields.shape), found.reshape(wet_land.shape), left.reshape(wet_land.shape)

    return jax.shard_map(
        on_device,
        mesh=mesh,
        in_specs=(
            P("tiles", "strip", None, None, None, None),
            P("tiles", "strip", None, None),
            P("tiles", "strip", None, None, None),
            P("tiles", "strip", None, None),
            P(),
            P(),
            P(),
        ),
        out_specs=(
            P("tiles", "strip", None, None, None, None),
            P("tiles", "strip", None, None),
            P("tiles", "strip", None, None),
        ),
        check_vma=False,
    )


def solution(mesh):
    return make(mesh, 32)
```
